32 devices in a mesh: row: 4 (over x, core), col: 4 (over z), layer: 2 (over y).
Axes of the slice: x: 2, y: 2, z: 4, core: 2. Of those that a mesh axis runs over, the one named last changes fastest.
Arguments:
- attn_values: bfloat16 [2048, 8192], P('row', ('layer', 'col')), may hold values from -6 to 6
- out_weight: bfloat16 [8192, 8192], P(('layer', 'row'), 'col'), may hold values from -0.09375 to 0.09375
Outputs:
- projected: bfloat16 [2048, 8192], P('row', ('col', 'layer'))
The draws below stay inside these ranges and needn't reach their ends.
All inputs are finite; a program needn't handle non-finite values.
Results may differ from the reference program's by a relative error of at most 0.001.
Values may be sent and summed in bfloat16 or wider, within the bound.
A program may use at most 128 MiB of HBM per device.

```python
import jax
import jax.numpy as jnp
from jax import lax

D = 8192
TOK_DEV = 512
TOKENS = 2048
N_ROW = 4


def with_spikes(entries, own_key, source, target, parts, factor):
    owner, partner = [(jnp.arange(entries.shape[axis_at]) // (entries.shape[axis_at] // parts)).reshape([-1 if axis == axis_at else 1 for axis in range(entries.ndim)]) for axis_at in (source, target)]
    chosen = jax.random.permutation(own_key, parts)[partner]
    strong = (owner == chosen) | (owner == (partner + parts // 2) % parts)
    return jnp.where(strong, factor * entries, entries)


def levels(stream_key, extent, pieces, low, high):
    loudness, own = 1.0, jax.random.fold_in(stream_key, 6)
    for axis_at, blocks in pieces:
        heights = jnp.exp(jax.random.uniform(jax.random.fold_in(own, axis_at), (blocks,), jnp.float32, low / len(pieces), high / len(pieces)))
        loudness = loudness * jnp.repeat(heights, extent[axis_at] // blocks).reshape([-1 if axis == axis_at else 1 for axis in range(len(extent))])
    return loudness


def noise(rng, dims, spread, bound, cuts=(), kind=jnp.bfloat16):
    loudness = levels(rng, dims, cuts, -0.22, 0.18) if cuts else 1.0
    entries = jax.random.normal(rng, dims, jnp.float32) * spread * loudness
    return jnp.minimum(jnp.maximum(entries, -bound), bound).astype(kind)


def bell_draw_with(rng, dims, spread, bound, shards, heavy, held_as=jnp.bfloat16):
    array = spread * jax.random.normal(rng, dims, jnp.float32)
    if shards:
        array = array * levels(rng, dims, shards, -0.22, 0.18)
    return jnp.clip(with_spikes(array, jax.random.fold_in(rng, 3), *heavy), -bound, bound).astype(held_as)


def setup_inputs(seed: int = 0) -> dict:
    seeds = jax.random.split(jax.random.key(seed), 3)
    return {
        "attn_values": noise(seeds[0], (TOKENS, D), 1.0, 6.0, ((0, 4), (1, 8))),
        "out_weight": bell_draw_with(seeds[1], (D, D), D ** -0.5, 0.09375, ((0, 8), (1, 4)), (0, 1, 8, 2.0)),
    }


def reference(attn_values, out_weight):
    token_blocks = attn_values.reshape(N_ROW, TOK_DEV, D)
    half_depth = D // 2

    def project(block):
        lower_part = jnp.dot(block[:, :half_depth], out_weight[:half_depth], preferred_element_type=jnp.float32)
        upper_part = jnp.dot(block[:, half_depth:], out_weight[half_depth:], preferred_element_type=jnp.float32)
        return (lower_part + upper_part).astype(jnp.bfloat16)

    return lax.map(project, token_blocks).reshape(TOK_DEV * N_ROW, D)
```

```python
import functools

import jax
import jax.numpy as jnp
from jax import lax
from jax.experimental import pallas as pl
from jax.experimental.pallas import tpu as pltpu
from jax.sharding import PartitionSpec as P

TOKEN_CHUNKS = 4
COLUMN_CHUNKS = 8


def last_pieces(depth_w):
    return max(1, min(4, depth_w // 256))


def schedule(token_chunks, column_chunks, col_count):
    events = []
    for t in range(token_chunks):
        for d in range(1, col_count):
            at = (col_count - 1) * t + (1 if d == 1 else d + 1)
            events.append((at, 0, t, d))
    span = (col_count - 1) * token_chunks * 4 / 3
    for j in range(column_chunks - 1):
        events.append((span * (j + 1) / column_chunks, 1, j, 0))
    ordered, clock = [], 0
    for at, kind, first, second in sorted(events, key=lambda e: (e[1], e[2], e[3])):
        if kind == 0:
            clock = max(clock, at)
            at = clock
        ordered.append((at, kind, first, second))
    return sorted(ordered)


def kernel(rows, cols, a_ref, w_ref, o_ref, abuf, wbuf, ysend, yrecv, early, loc_a, loc_w, a_recv, a_right, a_left, w_recv, w_send, p_send, y_recv, y_send):
    r, c, l = lax.axis_index("row"), lax.axis_index("col"), lax.axis_index("layer")
    groups = rows // 2
    core, group = lax.rem(r, 2), r // 2
    partner = 2 * group + 1 - core
    tokens, depth_a = a_ref.shape
    depth_w, width = w_ref.shape
    tt, half = tokens // TOKEN_CHUNKS, width // 2
    nc, jh = width // COLUMN_CHUNKS, COLUMN_CHUNKS // 2
    last, cuts = COLUMN_CHUNKS - 1, last_pieces(depth_w)
    pieces = last + cuts

    def piece(p):
        return (p, 0, depth_w) if p < last else (last, (p - last) * depth_w // cuts, depth_w // cuts)

    def peer(g):
        return 2 * lax.rem(group + g + groups, groups) + core

    def a_at(block, t):
        return abuf.at[block, pl.ds(t * tt, tt), :]

    def w_at(row, p):
        j, start, count = piece(p)
        return wbuf.at[j, pl.ds(pl.multiple_of(row * depth_w + start, count), count), :]

    def own_a(t):
        return pltpu.make_async_copy(a_ref.at[pl.ds(t * tt, tt), :], a_at(c, t), loc_a.at[t])

    def own_w(p):
        j, start, count = piece(p)
        side = 1 - l if j < jh else l
        at = pl.multiple_of(side * half + (j % jh) * nc, nc)
        return pltpu.make_async_copy(w_ref.at[pl.ds(start, count), pl.ds(at, nc)], w_at(r, p), loc_w.at[p])

    def a_copy(block, t, to, sems):
        return pltpu.make_async_remote_copy(a_at(block, t), a_at(block, t), sems.at[t, block], a_recv.at[t, block], device_id={"col": to})

    def w_copy(row, j, to, sem):
        return pltpu.make_async_remote_copy(w_at(row, j), w_at(row, j), sem, w_recv.at[j, row], device_id={"row": to})

    def y_copy(t, j):
        rows_t = pl.ds(t * tt, tt)
        return pltpu.make_async_remote_copy(ysend.at[j, rows_t, :], yrecv.at[j, rows_t, :], y_send.at[t, j], y_recv.at[t, j], device_id={"layer": 1 - l})

    def right(block, t):
        return a_copy(block, t, c + 1, a_right)

    def left(block, t):
        return a_copy(block, t, c - 1, a_left)

    for n in range(max(TOKEN_CHUNKS, pieces)):
        if n < pieces:
            own_w(n).start()
        if n < TOKEN_CHUNKS:
            own_a(n).start()

    has_right, has_left = c < cols - 1, c > 0
    barrier = pltpu.get_barrier_semaphore()

    def greet(device_id):
        pl.semaphore_signal(barrier, inc=1, device_id=device_id)

    greet({"row": partner})
    greet({"layer": 1 - l})
    for g in range(1, groups):
        greet({"row": peer(g)})
    pl.when(has_right)(lambda: greet({"col": c + 1}))
    pl.when(has_left)(lambda: greet({"col": c - 1}))
    pl.semaphore_wait(barrier, 1 + groups + has_right.astype(jnp.int32) + has_left.astype(jnp.int32))

    def send_a(t):
        own_a(t).wait()
        pl.when(has_right)(lambda: right(c, t).start())
        pl.when(has_left)(lambda: left(c, t).start())

    def send_w(j):
        own_w(j).wait()
        for g in range(1, groups):
            w_copy(r, j, peer(g), w_send.at[j, g]).start()
        w_copy(r, j, partner, p_send.at[j, 0]).start()

    send_w(0)
    send_a(0)
    send_a(1)
    for p in range(1, pieces):
        send_w(p)

    def take_a(t, d):
        @pl.when(c >= d)
        def _():
            right(c - d, t).wait_recv()
            pl.when(has_right)(lambda: right(c - d, t).start())

        @pl.when(c + d < cols)
        def _():
            left(c + d, t).wait_recv()
            pl.when(has_left)(lambda: left(c + d, t).start())

        if d == cols - 1 and t + 2 < TOKEN_CHUNKS:
            send_a(t + 2)

    def take_w(j):
        for g in range(1, groups):
            source = peer(-g)
            w_copy(source, j, partner, p_send.at[j, g]).wait_recv()
            w_copy(source, j, partner, p_send.at[j, g]).start()

    def take_partner(j):
        for g in range(groups):
            source = 2 * g + 1 - core
            w_copy(source, j, partner, p_send.at[j, 0]).wait_recv()

    def product(rows_t, j):
        total = jnp.dot(abuf[0, rows_t, :], wbuf[j, pl.ds(0, depth_a), :], preferred_element_type=jnp.float32)
        for block in range(1, cols):
            total += jnp.dot(abuf[block, rows_t, :], wbuf[j, pl.ds(block * depth_a, depth_a), :], preferred_element_type=jnp.float32)
        return total

    def partials(tiles):
        t0, j0 = tiles[0]
        wide = 1 + tiles[-1][1] - j0

        def one(n, carry):
            t, j = t0 + n // wide, j0 + lax.rem(n, wide)
            rows_t = pl.ds(pl.multiple_of(t * tt, tt), tt)
            ysend[j, rows_t, :] = product(rows_t, j)
            return carry

        def send(n, carry):
            y_copy(t0 + n // wide, j0 + lax.rem(n, wide)).start()
            return carry

        lax.fori_loop(0, len(tiles), one, 0)
        lax.fori_loop(0, len(tiles), send, 0)

    def finish(j):
        def one(t, carry):
            rows_t = pl.ds(pl.multiple_of(t * tt * 2, tt * 2), tt * 2)
            y_copy(2 * t, j - jh).wait_recv()
            y_copy(2 * t + 1, j - jh).wait_recv()
            o_ref[rows_t, (j - jh) * nc:(j - jh + 1) * nc] = (product(rows_t, j) + yrecv[j - jh, rows_t, :]).astype(o_ref.dtype)
            return carry

        lax.fori_loop(0, TOKEN_CHUNKS // 2, one, 0)

    def part(j, rows_t, start, count):
        columns = pl.ds(pl.multiple_of(lax.rem(start, depth_a), min(count, depth_a)), count)
        weights = wbuf[j, pl.ds(pl.multiple_of(start, count), count), :]
        return jnp.dot(abuf[start // depth_a, rows_t, columns], weights, preferred_element_type=jnp.float32)

    def each_rows(body):
        def one(t, carry):
            body(pl.ds(pl.multiple_of(t * tt * 2, tt * 2), tt * 2))
            return carry

        lax.fori_loop(0, TOKEN_CHUNKS // 2, one, 0)

    def take_own_rows():
        for h in range(cuts):
            w_copy(partner, last + h, partner, p_send.at[last + h, 0]).wait_recv()
        count = min(depth_w, depth_a)
        for n in range(depth_w // count):
            @each_rows
            def _(rows_t):
                total = part(last, rows_t, r * depth_w + n * count, count) + part(last, rows_t, partner * depth_w + n * count, count)
                early[rows_t, :] = total if n == 0 else early[rows_t, :] + total

    def finish_last():
        count = depth_w // cuts
        for t in range(TOKEN_CHUNKS):
            y_copy(t, jh - 1).wait_recv()
        for h in range(cuts):
            take_w(last + h)
            for g in range(1, groups):
                own, other = peer(-g), peer(-g) + 1 - 2 * core

                @each_rows
                def _(rows_t):
                    early[rows_t, :] += part(last, rows_t, own * depth_w + h * count, count)

                w_copy(other, last + h, partner, p_send.at[last + h, 0]).wait_recv()

                @each_rows
                def _(rows_t):
                    total = early[rows_t, :] + part(last, rows_t, other * depth_w + h * count, count)
                    if h < cuts - 1 or g < groups - 1:
                        early[rows_t, :] = total
                    else:
                        o_ref[rows_t, (jh - 1) * nc:jh * nc] = (total + yrecv[jh - 1, rows_t, :]).astype(o_ref.dtype)

    got_t, got_j, done_own, own_rows = 0, 0, jh, False
    for _, kind, first, second in schedule(TOKEN_CHUNKS, COLUMN_CHUNKS, cols):
        if kind == 0:
            take_a(first, second)
            if second == cols - 1:
                got_t = first + 1
                if got_j:
                    partials([(first, j) for j in range(min(got_j, jh))])
        else:
            if first == last - 1 and got_t == TOKEN_CHUNKS:
                take_own_rows()
                own_rows = True
            take_w(first)
            take_partner(first)
            got_j = first + 1
            if first < jh and got_t:
                partials([(t, first) for t in range(got_t)])
        while got_t == TOKEN_CHUNKS and done_own < got_j:
            finish(done_own)
            done_own += 1
    if not own_rows:
        take_own_rows()
    finish_last()

    for t in range(TOKEN_CHUNKS):
        for block in range(cols):
            @pl.when(has_right & (block <= c))
            def _():
                right(block, t).wait_send()

            @pl.when(has_left & (block >= c))
            def _():
                left(block, t).wait_send()

        for j in range(jh):
            y_copy(t, j).wait_send()
    for p in range(pieces):
        for g in range(groups):
            w_copy(r, p, partner, p_send.at[p, g]).wait_send()
            if g:
                w_copy(r, p, partner, w_send.at[p, g]).wait_send()


PIECES = 16
SPAN = 250.0


def pair_kernel(rows, cols, a_ref, w_ref, o_ref, abuf, wbuf, acc, part, ysend, yrecv, xsend, xrecv, loc_a, loc_w, a_recv, f_send, b_send, c_send, w_send, w_recv, y_send, y_recv, x_send, x_recv):
    r, c, l = lax.axis_index("row"), lax.axis_index("col"), lax.axis_index("layer")
    x, core = r // 2, lax.rem(r, 2)
    partner, peer = 2 * x + 1 - core, 2 * (1 - x) + core
    step, u, far = 1 - 2 * x, c + x * (cols - 1 - 2 * c), cols - 1
    own = core + x * (1 - 2 * core)
    tokens, depth = a_ref.shape
    half = w_ref.shape[1] // 2
    tt, nc = tokens // PIECES, wbuf.shape[3]
    tiles = half // nc
    lead = min(4, PIECES)

    def rows_at(t, side):
        return pl.ds(pl.multiple_of((2 * t + side) * tt, tt), tt)

    def rows_of(t):
        return pl.ds(pl.multiple_of(t * tt, tt), tt)

    def a_at(v, side, t):
        return abuf.at[v, rows_at(t, side), :]

    def own_a(t):
        return pltpu.make_async_copy(a_ref.at[rows_of(t), :], a_at(u - u // far, 0, t), loc_a.at[t])

    def own_w(j):
        side = 1 - l if j < tiles else l
        at = pl.multiple_of(side * half + (j % tiles) * nc, nc)
        return pltpu.make_async_copy(w_ref.at[:, pl.ds(at, nc)], wbuf.at[own, j], loc_w.at[j])

    def w_copy(slot, j):
        return pltpu.make_async_remote_copy(wbuf.at[slot, j], wbuf.at[slot, j], w_send.at[j], w_recv.at[j], device_id={"row": partner})

    def ahead(v, side, t):
        return pltpu.make_async_remote_copy(a_at(v, side, t), a_at(v, side, t), f_send.at[v + 2 * side, t], a_recv.at[v, side, t], device_id={"col": c + step})

    def back(v, side, t):
        return pltpu.make_async_remote_copy(a_at(v, side, t), a_at(v, side, t), b_send.at[v - 1 + 2 * side, t], a_recv.at[v, side, t], device_id={"col": c - step})

    def across(t):
        to = 1 - u // far
        return pltpu.make_async_remote_copy(a_at(2, 0, t), a_at(to, 1, t), c_send.at[t], a_recv.at[to, 1, t], device_id={"row": peer})

    def y_copy(t, side):
        at = rows_at(t, side)
        return pltpu.make_async_remote_copy(ysend.at[at, :], yrecv.at[at, :], y_send.at[t, side], y_recv.at[t, side], device_id={"layer": 1 - l})

    def x_copy(t):
        at = rows_of(t)
        return pltpu.make_async_remote_copy(xsend.at[at, :], xrecv.at[at, :], x_send.at[t], x_recv.at[t], device_id={"row": peer})

    def take(v, side, t):
        ahead(v, side, t).wait_recv()

    def within(t, body):
        pl.when(t < PIECES)(lambda: body(t))

    for t in range(PIECES):
        own_a(t).start()
    for j in range(2 * tiles):
        own_w(j).start()

    has_next, has_last = u < far, u > 0
    barrier = pltpu.get_barrier_semaphore()

    def greet(device_id):
        pl.semaphore_signal(barrier, inc=1, device_id=device_id)

    greet({"row": partner})
    greet({"row": peer})
    greet({"layer": 1 - l})
    pl.when(has_next)(lambda: greet({"col": c + step}))
    pl.when(has_last)(lambda: greet({"col": c - step}))
    pl.semaphore_wait(barrier, 3 + has_next.astype(jnp.int32) + has_last.astype(jnp.int32))

    def send_first(t):
        own_a(t).wait()
        ahead(0, 0, t).start()

    def send_second(t):
        own_a(t).wait()
        ahead(1, 0, t).start()
        back(1, 0, t).start()

    @pl.when(u == 0)
    def _():
        for t in range(lead):
            send_first(t)

    @pl.when(u == 1)
    def _():
        for t in range(lead):
            send_second(t)

    @pl.when(u == 2)
    def _():
        for t in range(PIECES):
            own_a(t).wait()
            across(t).start()
            back(2, 0, t).start()

    @pl.when(u == far)
    def _():
        for t in range(PIECES):
            own_a(t).wait()
            across(t).start()

    for j in range(2 * tiles):
        own_w(j).wait()
        w_copy(own, j).start()

    def pass_first(t):
        take(0, 1, t)
        ahead(0, 1, t).start()

    def pass_back(t):
        take(2, 0, t)
        back(2, 0, t).start()
        across(t).start()
        take(1, 1, t)
        back(1, 1, t).start()

    def pass_on(t):
        take(0, 0, t)
        ahead(0, 0, t).start()
        take(0, 1, t)
        ahead(0, 1, t).start()

    @pl.when(u == 0)
    def _():
        for t in range(3):
            pass_first(t)

    @pl.when(u == 1)
    def _():
        for t in range(3):
            pass_back(t)
        for t in range(2):
            pass_on(t)

    def gather(t):
        @pl.when(u == 0)
        def _():
            within(t + 3, pass_first)
            within(t + lead, send_first)
            take(1, 0, t)
            take(2, 0, t)
            across(t).start()
            take(1, 1, t)

        @pl.when(u == 1)
        def _():
            within(t + 3, pass_back)
            within(t + lead, send_second)
            within(t + 2, pass_on)

        @pl.when(u == 2)
        def _():
            for v, side in ((1, 0), (0, 0), (0, 1)):
                take(v, side, t)
                ahead(v, side, t).start()
            take(1, 1, t)

        @pl.when(u == far)
        def _():
            for v, side in ((1, 0), (0, 0), (0, 1), (1, 1)):
                take(v, side, t)

    def encode(ref, at, value):
        scale = jnp.maximum(1.01 * jnp.max(jnp.abs(value), axis=1, keepdims=True), 1e-30).astype(jnp.bfloat16)
        level = jnp.exp2(jnp.abs(value) * (SPAN / scale.astype(jnp.float32)) - SPAN / 2)
        ref[at, :half] = jnp.where(value < 0, -level, level).astype(jnp.bfloat16)
        ref[at, half:] = jnp.broadcast_to(scale, (value.shape[0], ref.shape[1] - half))

    def decode(ref, at):
        level = ref[at, :half].astype(jnp.float32)
        scale = ref[at, half:half + 1].astype(jnp.float32)
        share = jnp.log2(jnp.abs(level)) * (1 / SPAN) + 0.5
        return jnp.where(level < 0, -share, share) * scale

    def multiply(t):
        at = pl.ds(pl.multiple_of(2 * t * tt, 2 * tt), 2 * tt)
        first, second = abuf[0, at, :], abuf[1, at, :]
        for j in range(2 * tiles):
            @pl.when(t == 0)
            def _():
                w_copy(1 - own, j).wait_recv()

            total = jnp.dot(first, wbuf[0, j], preferred_element_type=jnp.float32) + jnp.dot(second, wbuf[1, j], preferred_element_type=jnp.float32)
            columns = pl.ds((j % tiles) * nc, nc)
            if j < tiles:
                part[:, columns] = total
            else:
                acc[at, columns] = total
        for side in (1, 0):
            encode(ysend, rows_at(t, side), part[side * tt:(side + 1) * tt, :])
        for side in (1, 0):
            y_copy(t, side).start()

    def reduce_y(t):
        y_copy(t, 1).wait_recv()
        at = rows_at(t, 1)
        encode(xsend, rows_of(t), acc[at, :] + decode(yrecv, at))
        x_copy(t).start()
        y_copy(t, 0).wait_recv()
        at = rows_at(t, 0)
        acc[at, :] += decode(yrecv, at)

    def reduce_x(t):
        x_copy(t).wait_recv()
        o_ref[rows_of(t), :] = (acc[rows_at(t, 0), :] + decode(xrecv, rows_of(t))).astype(o_ref.dtype)

    def one(t, carry):
        gather(t)
        multiply(t)
        pl.when(t >= 2)(lambda: reduce_y(t - 2))
        pl.when(t >= 3)(lambda: reduce_x(t - 3))
        return carry

    lax.fori_loop(0, PIECES, one, 0)
    reduce_y(PIECES - 2)
    reduce_y(PIECES - 1)
    for t in range(PIECES - 3, PIECES):
        reduce_x(t)

    def settle(t, carry):
        @pl.when(has_next)
        def _():
            ahead(0, 0, t).wait_send()
            ahead(0, 1, t).wait_send()
            pl.when(has_last)(lambda: ahead(1, 0, t).wait_send())

        @pl.when(u == 1)
        def _():
            back(1, 0, t).wait_send()
            back(1, 1, t).wait_send()

        pl.when(has_last & has_next)(lambda: back(2, 0, t).wait_send())
        across(t).wait_send()
        y_copy(t, 0).wait_send()
        y_copy(t, 1).wait_send()
        x_copy(t).wait_send()
        return carry

    lax.fori_loop(0, PIECES, settle, 0)
    for j in range(2 * tiles):
        w_copy(own, j).wait_send()


def pair_call(rows, cols, attn_values, out_weight):
    tokens, depth = attn_values.shape
    width = out_weight.shape[1]
    half = width // 2
    nc = half // 4
    dma = pltpu.SemaphoreType.DMA
    return pl.pallas_call(
        functools.partial(pair_kernel, rows, cols),
        out_shape=jax.ShapeDtypeStruct((tokens, half), jnp.bfloat16),
        in_specs=[pl.BlockSpec(memory_space=pltpu.HBM)] * 2,
        out_specs=pl.BlockSpec(memory_space=pltpu.VMEM),
        scratch_shapes=[
            pltpu.VMEM((3, 2 * tokens, depth), jnp.bfloat16),
            pltpu.VMEM((2, width // nc, depth, nc), jnp.bfloat16),
            pltpu.VMEM((2 * tokens, half), jnp.float32),
            pltpu.VMEM((2 * tokens // PIECES, half), jnp.float32),
            pltpu.VMEM((2 * tokens, half + 128), jnp.bfloat16),
            pltpu.VMEM((2 * tokens, half + 128), jnp.bfloat16),
            pltpu.VMEM((tokens, half + 128), jnp.bfloat16),
            pltpu.VMEM((tokens, half + 128), jnp.bfloat16),
            dma((PIECES,)),
            dma((width // nc,)),
            dma((3, 2, PIECES)),
            dma((3, PIECES)),
            dma((3, PIECES)),
            dma((PIECES,)),
            dma((width // nc,)),
            dma((width // nc,)),
            dma((PIECES, 2)),
            dma((PIECES, 2)),
            dma((PIECES,)),
            dma((PIECES,)),
        ],
        compiler_params=pltpu.CompilerParams(collective_id=1, has_side_effects=True, vmem_limit_bytes=48 * 2**20),
    )(*(pltpu.with_memory_space_constraint(v, pltpu.HBM) for v in (attn_values, out_weight)))


def solution(mesh):
    rows, cols = mesh.shape["row"], mesh.shape["col"]

    def shards(attn_values, out_weight):
        if rows == cols == 4:
            return pair_call(rows, cols, attn_values, out_weight)
        tokens, depth_a = attn_values.shape
        depth_w, width = out_weight.shape
        nc, jh = width // COLUMN_CHUNKS, COLUMN_CHUNKS // 2
        pieces = COLUMN_CHUNKS - 1 + last_pieces(depth_w)
        dma = pltpu.SemaphoreType.DMA
        return pl.pallas_call(
            functools.partial(kernel, rows, cols),
            out_shape=jax.ShapeDtypeStruct((tokens, width // 2), jnp.bfloat16),
            in_specs=[pl.BlockSpec(memory_space=pltpu.HBM)] * 2,
            out_specs=pl.BlockSpec(memory_space=pltpu.VMEM),
            scratch_shapes=[
                pltpu.VMEM((cols, tokens, depth_a), jnp.bfloat16),
                pltpu.VMEM((COLUMN_CHUNKS, rows * depth_w, nc), jnp.bfloat16),
                pltpu.VMEM((jh, tokens, nc), jnp.float32),
                pltpu.VMEM((jh, tokens, nc), jnp.float32),
                pltpu.VMEM((tokens, nc), jnp.float32),
                dma((TOKEN_CHUNKS,)),
                dma((pieces,)),
                dma((TOKEN_CHUNKS, cols)),
                dma((TOKEN_CHUNKS, cols)),
                dma((TOKEN_CHUNKS, cols)),
                dma((pieces, rows)),
                dma((pieces, rows // 2)),
                dma((pieces, rows // 2)),
                dma((TOKEN_CHUNKS, jh)),
                dma((TOKEN_CHUNKS, jh)),
            ],
            compiler_params=pltpu.CompilerParams(collective_id=0, has_side_effects=True, vmem_limit_bytes=48 * 2**20),
        )(*(pltpu.with_memory_space_constraint(x, pltpu.HBM) for x in (attn_values, out_weight)))

    in_specs = (P("row", ("layer", "col")), P(("layer", "row"), "col"))
    out_specs = P("row", ("col", "layer"))
    return jax.shard_map(shards, mesh=mesh, in_specs=in_specs, out_specs=out_specs, check_vma=False)
```

```python
import functools

import jax
import jax.numpy as jnp
from jax import lax
from jax.experimental import pallas as pl
from jax.experimental.pallas import tpu as pltpu
from jax.sharding import PartitionSpec as P

TOKEN_CHUNKS = 4
COLUMN_CHUNKS = 8


def last_pieces(depth_w):
    return max(1, min(4, depth_w // 256))


def schedule(token_chunks, column_chunks, col_count):
    events = []
    for t in range(token_chunks):
        for d in range(1, col_count):
            at = (col_count - 1) * t + (1 if d == 1 else d + 1)
            events.append((at, 0, t, d))
    span = (col_count - 1) * token_chunks * 4 / 3
    for j in range(column_chunks - 1):
        events.append((span * (j + 1) / column_chunks, 1, j, 0))
    ordered, clock = [], 0
    for at, kind, first, second in sorted(events, key=lambda e: (e[1], e[2], e[3])):
        if kind == 0:
            clock = max(clock, at)
            at = clock
        ordered.append((at, kind, first, second))
    return sorted(ordered)


def kernel(rows, cols, a_ref, w_ref, o_ref, abuf, wbuf, ysend, yrecv, early, loc_a, loc_w, a_recv, a_right, a_left, w_recv, w_send, p_send, y_recv, y_send):
    r, c, l = lax.axis_index("row"), lax.axis_index("col"), lax.axis_index("layer")
    groups = rows // 2
    core, group = lax.rem(r, 2), r // 2
    partner = 2 * group + 1 - core
    tokens, depth_a = a_ref.shape
    depth_w, width = w_ref.shape
    tt, half = tokens // TOKEN_CHUNKS, width // 2
    nc, jh = width // COLUMN_CHUNKS, COLUMN_CHUNKS // 2
    last, cuts = COLUMN_CHUNKS - 1, last_pieces(depth_w)
    pieces = last + cuts

    def piece(p):
        return (p, 0, depth_w) if p < last else (last, (p - last) * depth_w // cuts, depth_w // cuts)

    def peer(g):
        return 2 * lax.rem(group + g + groups, groups) + core

    def a_at(block, t):
        return abuf.at[block, pl.ds(t * tt, tt), :]

    def w_at(row, p):
        j, start, count = piece(p)
        return wbuf.at[j, pl.ds(pl.multiple_of(row * depth_w + start, count), count), :]

    def own_a(t):
        return pltpu.make_async_copy(a_ref.at[pl.ds(t * tt, tt), :], a_at(c, t), loc_a.at[t])

    def own_w(p):
        j, start, count = piece(p)
        side = 1 - l if j < jh else l
        at = pl.multiple_of(side * half + (j % jh) * nc, nc)
        return pltpu.make_async_copy(w_ref.at[pl.ds(start, count), pl.ds(at, nc)], w_at(r, p), loc_w.at[p])

    def a_copy(block, t, to, sems):
        return pltpu.make_async_remote_copy(a_at(block, t), a_at(block, t), sems.at[t, block], a_recv.at[t, block], device_id={"col": to})

    def w_copy(row, j, to, sem):
        return pltpu.make_async_remote_copy(w_at(row, j), w_at(row, j), sem, w_recv.at[j, row], device_id={"row": to})

    def y_copy(t, j):
        rows_t = pl.ds(t * tt, tt)
        return pltpu.make_async_remote_copy(ysend.at[j, rows_t, :], yrecv.at[j, rows_t, :], y_send.at[t, j], y_recv.at[t, j], device_id={"layer": 1 - l})

    def right(block, t):
        return a_copy(block, t, c + 1, a_right)

    def left(block, t):
        return a_copy(block, t, c - 1, a_left)

    for n in range(max(TOKEN_CHUNKS, pieces)):
        if n < pieces:
            own_w(n).start()
        if n < TOKEN_CHUNKS:
            own_a(n).start()

    has_right, has_left = c < cols - 1, c > 0
    barrier = pltpu.get_barrier_semaphore()

    def greet(device_id):
        pl.semaphore_signal(barrier, inc=1, device_id=device_id)

    greet({"row": partner})
    greet({"layer": 1 - l})
    for g in range(1, groups):
        greet({"row": peer(g)})
    pl.when(has_right)(lambda: greet({"col": c + 1}))
    pl.when(has_left)(lambda: greet({"col": c - 1}))
    pl.semaphore_wait(barrier, 1 + groups + has_right.astype(jnp.int32) + has_left.astype(jnp.int32))

    def send_a(t):
        own_a(t).wait()
        pl.when(has_right)(lambda: right(c, t).start())
        pl.when(has_left)(lambda: left(c, t).start())

    def send_w(j):
        own_w(j).wait()
        for g in range(1, groups):
            w_copy(r, j, peer(g), w_send.at[j, g]).start()
        w_copy(r, j, partner, p_send.at[j, 0]).start()

    send_w(0)
    send_a(0)
    send_a(1)
    for p in range(1, pieces):
        send_w(p)

    def take_a(t, d):
        @pl.when(c >= d)
        def _():
            right(c - d, t).wait_recv()
            pl.when(has_right)(lambda: right(c - d, t).start())

        @pl.when(c + d < cols)
        def _():
            left(c + d, t).wait_recv()
            pl.when(has_left)(lambda: left(c + d, t).start())

        if d == cols - 1 and t + 2 < TOKEN_CHUNKS:
            send_a(t + 2)

    def take_w(j):
        for g in range(1, groups):
            source = peer(-g)
            w_copy(source, j, partner, p_send.at[j, g]).wait_recv()
            w_copy(source, j, partner, p_send.at[j, g]).start()

    def take_partner(j):
        for g in range(groups):
            source = 2 * g + 1 - core
            w_copy(source, j, partner, p_send.at[j, 0]).wait_recv()

    def product(rows_t, j):
        total = jnp.dot(abuf[0, rows_t, :], wbuf[j, pl.ds(0, depth_a), :], preferred_element_type=jnp.float32)
        for block in range(1, cols):
            total += jnp.dot(abuf[block, rows_t, :], wbuf[j, pl.ds(block * depth_a, depth_a), :], preferred_element_type=jnp.float32)
        return total

    def partials(tiles):
        t0, j0 = tiles[0]
        wide = 1 + tiles[-1][1] - j0

        def one(n, carry):
            t, j = t0 + n // wide, j0 + lax.rem(n, wide)
            rows_t = pl.ds(pl.multiple_of(t * tt, tt), tt)
            ysend[j, rows_t, :] = product(rows_t, j)
            return carry

        def send(n, carry):
            y_copy(t0 + n // wide, j0 + lax.rem(n, wide)).start()
            return carry

        lax.fori_loop(0, len(tiles), one, 0)
        lax.fori_loop(0, len(tiles), send, 0)

    def finish(j):
        def one(t, carry):
            rows_t = pl.ds(pl.multiple_of(t * tt * 2, tt * 2), tt * 2)
            y_copy(2 * t, j - jh).wait_recv()
            y_copy(2 * t + 1, j - jh).wait_recv()
            o_ref[rows_t, (j - jh) * nc:(j - jh + 1) * nc] = (product(rows_t, j) + yrecv[j - jh, rows_t, :]).astype(o_ref.dtype)
            return carry

        lax.fori_loop(0, TOKEN_CHUNKS // 2, one, 0)

    def part(j, rows_t, start, count):
        columns = pl.ds(pl.multiple_of(lax.rem(start, depth_a), min(count, depth_a)), count)
        weights = wbuf[j, pl.ds(pl.multiple_of(start, count), count), :]
        return jnp.dot(abuf[start // depth_a, rows_t, columns], weights, preferred_element_type=jnp.float32)

    def each_rows(body):
        def one(t, carry):
            body(pl.ds(pl.multiple_of(t * tt * 2, tt * 2), tt * 2))
            return carry

        lax.fori_loop(0, TOKEN_CHUNKS // 2, one, 0)

    def take_own_rows():
        for h in range(cuts):
            w_copy(partner, last + h, partner, p_send.at[last + h, 0]).wait_recv()
        count = min(depth_w, depth_a)
        for n in range(depth_w // count):
            @each_rows
            def _(rows_t):
                total = part(last, rows_t, r * depth_w + n * count, count) + part(last, rows_t, partner * depth_w + n * count, count)
                early[rows_t, :] = total if n == 0 else early[rows_t, :] + total

    def finish_last():
        count = depth_w // cuts
        for t in range(TOKEN_CHUNKS):
            y_copy(t, jh - 1).wait_recv()
        for h in range(cuts):
            take_w(last + h)
            for g in range(1, groups):
                own, other = peer(-g), peer(-g) + 1 - 2 * core

                @each_rows
                def _(rows_t):
                    early[rows_t, :] += part(last, rows_t, own * depth_w + h * count, count)

                w_copy(other, last + h, partner, p_send.at[last + h, 0]).wait_recv()

                @each_rows
                def _(rows_t):
                    total = early[rows_t, :] + part(last, rows_t, other * depth_w + h * count, count)
                    if h < cuts - 1 or g < groups - 1:
                        early[rows_t, :] = total
                    else:
                        o_ref[rows_t, (jh - 1) * nc:jh * nc] = (total + yrecv[jh - 1, rows_t, :]).astype(o_ref.dtype)

    got_t, got_j, done_own, own_rows = 0, 0, jh, False
    for _, kind, first, second in schedule(TOKEN_CHUNKS, COLUMN_CHUNKS, cols):
        if kind == 0:
            take_a(first, second)
            if second == cols - 1:
                got_t = first + 1
                if got_j:
                    partials([(first, j) for j in range(min(got_j, jh))])
        else:
            if first == last - 1 and got_t == TOKEN_CHUNKS:
                take_own_rows()
                own_rows = True
            take_w(first)
            take_partner(first)
            got_j = first + 1
            if first < jh and got_t:
                partials([(t, first) for t in range(got_t)])
        while got_t == TOKEN_CHUNKS and done_own < got_j:
            finish(done_own)
            done_own += 1
    if not own_rows:
        take_own_rows()
    finish_last()

    for t in range(TOKEN_CHUNKS):
        for block in range(cols):
            @pl.when(has_right & (block <= c))
            def _():
                right(block, t).wait_send()

            @pl.when(has_left & (block >= c))
            def _():
                left(block, t).wait_send()

        for j in range(jh):
            y_copy(t, j).wait_send()
    for p in range(pieces):
        for g in range(groups):
            w_copy(r, p, partner, p_send.at[p, g]).wait_send()
            if g:
                w_copy(r, p, partner, w_send.at[p, g]).wait_send()


PIECES = 16
FILL = 6
FILL_BACK = 3
LEAD = 2
LAG_O = 1
LAG_Y = 2
LAG_X = 5
SPAN = 250.0


def pair_kernel(rows, cols, a_ref, w_ref, o_ref, abuf, wbuf, acc, part, ysend, yrecv, xsend, xrecv, loc_a, loc_w, a_recv, f_send, b_send, c_send, w_send, w_recv, y_send, y_recv, x_send, x_recv):
    r, c, l = lax.axis_index("row"), lax.axis_index("col"), lax.axis_index("layer")
    x, core = r // 2, lax.rem(r, 2)
    partner, peer = 2 * x + 1 - core, 2 * (1 - x) + core
    step, u, far = 1 - 2 * x, c + x * (cols - 1 - 2 * c), cols - 1
    own = core + x * (1 - 2 * core)
    tokens, depth = a_ref.shape
    half = w_ref.shape[1] // 2
    tt, nc = tokens // PIECES, wbuf.shape[3]
    tiles = half // nc

    def rows_at(t, side):
        at = 2 * t if side == 0 else 2 * lax.rem(t + PIECES - LEAD, PIECES) + 1
        return pl.ds(pl.multiple_of(at * tt, tt), tt)

    def rows_of(t):
        return pl.ds(pl.multiple_of(t * tt, tt), tt)

    def a_at(v, side, t):
        return abuf.at[v, rows_at(t, side), :]

    def a_all(v):
        return abuf.at[v, pl.ds(0, tokens), :]

    def own_a(t):
        return pltpu.make_async_copy(a_ref.at[rows_of(t), :], a_at(u - u // far, 0, t), loc_a)

    def own_w(j):
        side = 1 - l if j < tiles else l
        at = pl.multiple_of(side * half + (j % tiles) * nc, nc)
        return pltpu.make_async_copy(w_ref.at[:, pl.ds(at, nc)], wbuf.at[own, j], loc_w.at[j])

    def remote(source, target, sent, got, **device):
        return pltpu.make_async_remote_copy(source, target, sent, got, device_id=device)

    def w_copy(slot, j):
        return remote(wbuf.at[slot, j], wbuf.at[slot, j], w_send, w_recv, row=partner)

    def w_all(slot):
        return remote(wbuf.at[slot], wbuf.at[slot], w_send, w_recv, row=partner)

    def ahead(v, side, t):
        return remote(a_at(v, side, t), a_at(v, side, t), f_send.at[v + 2 * side], a_recv.at[v + 3 * side, t], col=c + step)

    def back(v, side, t):
        return remote(a_at(v, side, t), a_at(v, side, t), b_send.at[v - 1 + 2 * side], a_recv.at[v + 3 * side, t], col=c - step)

    def across(t):
        to = 1 - u // far
        return remote(a_at(2, 0, t), a_at(to, 1, t), c_send, a_recv.at[to + 3, t], row=peer)

    def y_copy(t, side):
        at = rows_at(t, side)
        return remote(ysend.at[at, :], yrecv.at[at, :], y_send, y_recv.at[t, side], layer=1 - l)

    def x_copy(t):
        at = rows_of(t)
        return remote(xsend.at[at, :], xrecv.at[at, :], x_send, x_recv.at[t], row=peer)

    def take(v, side, t):
        ahead(v, side, t).wait_recv()

    def within(first, t, body):
        if isinstance(t, int):
            if first <= t < PIECES:
                body(t)
        else:
            pl.when((t >= first) & (t < PIECES))(lambda: body(t))

    for t in range(PIECES):
        own_a(t).start()
    for j in range(2 * tiles):
        own_w(j).start()

    has_next, has_last = u < far, u > 0
    barrier = pltpu.get_barrier_semaphore()

    def greet(device_id):
        pl.semaphore_signal(barrier, inc=1, device_id=device_id)

    greet({"row": partner})
    greet({"row": peer})
    greet({"layer": 1 - l})
    pl.when(has_next)(lambda: greet({"col": c + step}))
    pl.when(has_last)(lambda: greet({"col": c - step}))
    pl.semaphore_wait(barrier, 3 + has_next.astype(jnp.int32) + has_last.astype(jnp.int32))

    pltpu.make_async_copy(a_ref, a_all(u - u // far), loc_a).wait()

    def send_first(t):
        ahead(0, 0, t).start()

    def send_ahead(t):
        ahead(1, 0, t).start()

    def send_back(t):
        back(1, 0, t).start()

    def each(start, stop, body):
        def one(t, carry):
            body(t)
            return carry

        lax.fori_loop(start, stop, one, 0)

    @pl.when(u == 0)
    def _():
        each(0, 2, send_first)

    @pl.when(u == 1)
    def _():
        for t in range(FILL):
            send_ahead(t)
            if t < FILL_BACK:
                send_back(t)

    @pl.when(u == 2)
    def _():
        def both(t):
            across(t).start()
            back(2, 0, t).start()

        each(0, PIECES, both)

    @pl.when(u == far)
    def _():
        each(0, PIECES, lambda t: across(t).start())

    for j in range(2 * tiles):
        own_w(j).wait()
        w_copy(own, j).start()

    def on(v, side):
        def body(t):
            take(v, side, t)
            ahead(v, side, t).start()

        return body

    def cross(t):
        take(2, 0, t)
        across(t).start()

    def pass_back(t):
        take(2, 0, t)
        back(2, 0, t).start()
        across(t).start()
        take(1, 1, t)
        back(1, 1, t).start()

    @pl.when(u == 0)
    def _():
        for t in range(4):
            on(0, 1)(t)
            if t >= 2:
                send_first(t)

    @pl.when(u == 1)
    def _():
        for t in range(3):
            pass_back(t)
        for t in range(2):
            on(0, 1)(t)

    @pl.when(u == 2)
    def _():
        for t in range(FILL):
            on(1, 0)(t)

    def gather(t):
        @pl.when(u == 0)
        def _():
            within(0, t + LEAD, cross)
            within(4, t + LEAD + 4, on(0, 1))
            within(4, t + 4, send_first)
            within(0, t + LEAD, lambda t: take(1, 1, t))
            within(0, t, lambda t: take(1, 0, t))

        @pl.when(u == 1)
        def _():
            within(3, t + LEAD + 3, pass_back)
            within(FILL_BACK, t + 3, send_back)
            within(2, t + LEAD + 2, on(0, 1))
            within(0, t + 2, on(0, 0))
            within(FILL, t + 2, send_ahead)

        @pl.when(u == 2)
        def _():
            within(0, t + LEAD, on(0, 1))
            within(0, t, on(0, 0))
            within(FILL, t, on(1, 0))
            within(0, t + LEAD, lambda t: take(1, 1, t))

        @pl.when(u == far)
        def _():
            within(0, t + LEAD, lambda t: take(0, 1, t))
            within(0, t + LEAD, lambda t: take(1, 1, t))
            within(0, t, lambda t: take(0, 0, t))
            within(0, t, lambda t: take(1, 0, t))

    def encode(ref, at, value):
        scale = jnp.maximum(1.01 * jnp.max(jnp.abs(value), axis=1, keepdims=True), 1e-30).astype(jnp.bfloat16)
        level = jnp.exp2(jnp.abs(value) * (SPAN / scale.astype(jnp.float32)) - SPAN / 2)
        ref[at, :half] = jnp.where(value < 0, -level, level).astype(jnp.bfloat16)
        ref[at, half:] = jnp.broadcast_to(scale, (value.shape[0], ref.shape[1] - half))

    def decode(ref, at):
        level = ref[at, :half].astype(jnp.float32)
        scale = ref[at, half:half + 1].astype(jnp.float32)
        share = jnp.log2(jnp.abs(level)) * (1 / SPAN) + 0.5
        return jnp.where(level < 0, -share, share) * scale

    def multiply(at, sends):
        first, second = abuf[0, at, :], abuf[1, at, :]

        def product(j):
            return jnp.dot(first, wbuf[0, j], preferred_element_type=jnp.float32) + jnp.dot(second, wbuf[1, j], preferred_element_type=jnp.float32)

        for j in range(tiles):
            part[:at.size, j * nc:(j + 1) * nc] = product(j)
        for t, side, start in sends:
            encode(ysend, rows_at(t, side), part[start:start + tt, :])
        for t, side, start in sends:
            y_copy(t, side).start()
        for j in range(tiles):
            acc[at, j * nc:(j + 1) * nc] = product(tiles + j)

    def reduce_other(t):
        y_copy(t, 1).wait_recv()
        at = rows_at(t, 1)
        encode(xsend, rows_of(t), acc[at, :] + decode(yrecv, at))
        x_copy(t).start()

    def reduce_own(t):
        y_copy(t, 0).wait_recv()
        at = rows_at(t, 0)
        acc[at, :] += decode(yrecv, at)

    def finish(t):
        x_copy(t).wait_recv()
        o_ref[rows_of(t), :] = (acc[rows_at(t, 0), :] + decode(xrecv, rows_of(t))).astype(o_ref.dtype)

    def reduce(t):
        within(0, t + LEAD - 1 - LAG_O, reduce_other)
        within(0, t - LAG_Y, reduce_own)
        within(0, t - LAG_X, finish)

    def early(t):
        gather(t)
        multiply(rows_at(t + LEAD, 1), [(t + LEAD, 1, 0)])
        reduce(t)

    def steady(t):
        gather(t)
        multiply(pl.ds(pl.multiple_of(2 * t * tt, 2 * tt), 2 * tt), [(t + LEAD, 1, tt), (t, 0, 0)])
        reduce(t)

    def late(t):
        gather(t)
        multiply(rows_at(t, 0), [(t, 0, 0)])
        reduce(t)

    w_all(1 - own).wait_recv()
    each(-LEAD, 0, early)
    each(0, PIECES - LEAD, steady)
    each(PIECES - LEAD, PIECES, late)
    each(PIECES, PIECES + LAG_X, reduce)

    def sent(sem):
        remote(a_all(0), a_all(0), sem, a_recv.at[0, 0], row=peer).wait_send()

    @pl.when(has_next)
    def _():
        sent(f_send.at[0])
        sent(f_send.at[2])
        pl.when(has_last)(lambda: sent(f_send.at[1]))

    @pl.when(u == 1)
    def _():
        sent(b_send.at[0])
        sent(b_send.at[2])

    pl.when(has_last & has_next)(lambda: sent(b_send.at[1]))
    sent(c_send)
    remote(ysend, yrecv, y_send, y_recv.at[0, 0], layer=1 - l).wait_send()
    remote(xsend, xrecv, x_send, x_recv.at[0], row=peer).wait_send()
    w_all(own).wait_send()


def pair_call(rows, cols, attn_values, out_weight):
    tokens, depth = attn_values.shape
    width = out_weight.shape[1]
    half = width // 2
    nc = half // 4
    dma = pltpu.SemaphoreType.DMA
    return pl.pallas_call(
        functools.partial(pair_kernel, rows, cols),
        out_shape=jax.ShapeDtypeStruct((tokens, half), jnp.bfloat16),
        in_specs=[pl.BlockSpec(memory_space=pltpu.HBM)] * 2,
        out_specs=pl.BlockSpec(memory_space=pltpu.VMEM),
        scratch_shapes=[
            pltpu.VMEM((3, 2 * tokens, depth), jnp.bfloat16),
            pltpu.VMEM((2, width // nc, depth, nc), jnp.bfloat16),
            pltpu.VMEM((2 * tokens, half), jnp.float32),
            pltpu.VMEM((2 * tokens // PIECES, half), jnp.float32),
            pltpu.VMEM((2 * tokens, half + 128), jnp.bfloat16),
            pltpu.VMEM((2 * tokens, half + 128), jnp.bfloat16),
            pltpu.VMEM((tokens, half + 128), jnp.bfloat16),
            pltpu.VMEM((tokens, half + 128), jnp.bfloat16),
            dma,
            dma((width // nc,)),
            dma((5, PIECES)),
            dma((3,)),
            dma((3,)),
            dma,
            dma,
            dma,
            dma,
            dma((PIECES, 2)),
            dma,
            dma((PIECES,)),
        ],
        compiler_params=pltpu.CompilerParams(collective_id=1, has_side_effects=True, vmem_limit_bytes=48 * 2**20),
    )(*(pltpu.with_memory_space_constraint(v, pltpu.HBM) for v in (attn_values, out_weight)))


def solution(mesh):
    rows, cols = mesh.shape["row"], mesh.shape["col"]

    def shards(attn_values, out_weight):
        if rows == cols == 4:
            return pair_call(rows, cols, attn_values, out_weight)
        tokens, depth_a = attn_values.shape
        depth_w, width = out_weight.shape
        nc, jh = width // COLUMN_CHUNKS, COLUMN_CHUNKS // 2
        pieces = COLUMN_CHUNKS - 1 + last_pieces(depth_w)
        dma = pltpu.SemaphoreType.DMA
        return pl.pallas_call(
            functools.partial(kernel, rows, cols),
            out_shape=jax.ShapeDtypeStruct((tokens, width // 2), jnp.bfloat16),
            in_specs=[pl.BlockSpec(memory_space=pltpu.HBM)] * 2,
            out_specs=pl.BlockSpec(memory_space=pltpu.VMEM),
            scratch_shapes=[
                pltpu.VMEM((cols, tokens, depth_a), jnp.bfloat16),
                pltpu.VMEM((COLUMN_CHUNKS, rows * depth_w, nc), jnp.bfloat16),
                pltpu.VMEM((jh, tokens, nc), jnp.float32),
                pltpu.VMEM((jh, tokens, nc), jnp.float32),
                pltpu.VMEM((tokens, nc), jnp.float32),
                dma((TOKEN_CHUNKS,)),
                dma((pieces,)),
                dma((TOKEN_CHUNKS, cols)),
                dma((TOKEN_CHUNKS, cols)),
                dma((TOKEN_CHUNKS, cols)),
                dma((pieces, rows)),
                dma((pieces, rows // 2)),
                dma((pieces, rows // 2)),
                dma((TOKEN_CHUNKS, jh)),
                dma((TOKEN_CHUNKS, jh)),
            ],
            compiler_params=pltpu.CompilerParams(collective_id=0, has_side_effects=True, vmem_limit_bytes=48 * 2**20),
        )(*(pltpu.with_memory_space_constraint(x, pltpu.HBM) for x in (attn_values, out_weight)))

    in_specs = (P("row", ("layer", "col")), P(("layer", "row"), "col"))
    out_specs = P("row", ("col", "layer"))
    return jax.shard_map(shards, mesh=mesh, in_specs=in_specs, out_specs=out_specs, check_vma=False)
```

```python
import functools

import jax
import jax.numpy as jnp
from jax import lax
from jax.experimental import pallas as pl
from jax.experimental.pallas import tpu as pltpu
from jax.sharding import PartitionSpec as P

TOKEN_CHUNKS = 4
COLUMN_CHUNKS = 8


def last_pieces(depth_w):
    return max(1, min(4, depth_w // 256))


def schedule(token_chunks, column_chunks, col_count):
    events = []
    for t in range(token_chunks):
        for d in range(1, col_count):
            at = (col_count - 1) * t + (1 if d == 1 else d + 1)
            events.append((at, 0, t, d))
    span = (col_count - 1) * token_chunks * 4 / 3
    for j in range(column_chunks - 1):
        events.append((span * (j + 1) / column_chunks, 1, j, 0))
    ordered, clock = [], 0
    for at, kind, first, second in sorted(events, key=lambda e: (e[1], e[2], e[3])):
        if kind == 0:
            clock = max(clock, at)
            at = clock
        ordered.append((at, kind, first, second))
    return sorted(ordered)


def kernel(rows, cols, a_ref, w_ref, o_ref, abuf, wbuf, ysend, yrecv, early, loc_a, loc_w, a_recv, a_right, a_left, w_recv, w_send, p_send, y_recv, y_send):
    r, c, l = lax.axis_index("row"), lax.axis_index("col"), lax.axis_index("layer")
    groups = rows // 2
    core, group = lax.rem(r, 2), r // 2
    partner = 2 * group + 1 - core
    tokens, depth_a = a_ref.shape
    depth_w, width = w_ref.shape
    tt, half = tokens // TOKEN_CHUNKS, width // 2
    nc, jh = width // COLUMN_CHUNKS, COLUMN_CHUNKS // 2
    last, cuts = COLUMN_CHUNKS - 1, last_pieces(depth_w)
    pieces = last + cuts

    def piece(p):
        return (p, 0, depth_w) if p < last else (last, (p - last) * depth_w // cuts, depth_w // cuts)

    def peer(g):
        return 2 * lax.rem(group + g + groups, groups) + core

    def a_at(block, t):
        return abuf.at[block, pl.ds(t * tt, tt), :]

    def w_at(row, p):
        j, start, count = piece(p)
        return wbuf.at[j, pl.ds(pl.multiple_of(row * depth_w + start, count), count), :]

    def own_a(t):
        return pltpu.make_async_copy(a_ref.at[pl.ds(t * tt, tt), :], a_at(c, t), loc_a.at[t])

    def own_w(p):
        j, start, count = piece(p)
        side = 1 - l if j < jh else l
        at = pl.multiple_of(side * half + (j % jh) * nc, nc)
        return pltpu.make_async_copy(w_ref.at[pl.ds(start, count), pl.ds(at, nc)], w_at(r, p), loc_w.at[p])

    def a_copy(block, t, to, sems):
        return pltpu.make_async_remote_copy(a_at(block, t), a_at(block, t), sems.at[t, block], a_recv.at[t, block], device_id={"col": to})

    def w_copy(row, j, to, sem):
        return pltpu.make_async_remote_copy(w_at(row, j), w_at(row, j), sem, w_recv.at[j, row], device_id={"row": to})

    def y_copy(t, j):
        rows_t = pl.ds(t * tt, tt)
        return pltpu.make_async_remote_copy(ysend.at[j, rows_t, :], yrecv.at[j, rows_t, :], y_send.at[t, j], y_recv.at[t, j], device_id={"layer": 1 - l})

    def right(block, t):
        return a_copy(block, t, c + 1, a_right)

    def left(block, t):
        return a_copy(block, t, c - 1, a_left)

    for n in range(max(TOKEN_CHUNKS, pieces)):
        if n < pieces:
            own_w(n).start()
        if n < TOKEN_CHUNKS:
            own_a(n).start()

    has_right, has_left = c < cols - 1, c > 0
    barrier = pltpu.get_barrier_semaphore()

    def greet(device_id):
        pl.semaphore_signal(barrier, inc=1, device_id=device_id)

    greet({"row": partner})
    greet({"layer": 1 - l})
    for g in range(1, groups):
        greet({"row": peer(g)})
    pl.when(has_right)(lambda: greet({"col": c + 1}))
    pl.when(has_left)(lambda: greet({"col": c - 1}))
    pl.semaphore_wait(barrier, 1 + groups + has_right.astype(jnp.int32) + has_left.astype(jnp.int32))

    def send_a(t):
        own_a(t).wait()
        pl.when(has_right)(lambda: right(c, t).start())
        pl.when(has_left)(lambda: left(c, t).start())

    def send_w(j):
        own_w(j).wait()
        for g in range(1, groups):
            w_copy(r, j, peer(g), w_send.at[j, g]).start()
        w_copy(r, j, partner, p_send.at[j, 0]).start()

    send_w(0)
    send_a(0)
    send_a(1)
    for p in range(1, pieces):
        send_w(p)

    def take_a(t, d):
        @pl.when(c >= d)
        def _():
            right(c - d, t).wait_recv()
            pl.when(has_right)(lambda: right(c - d, t).start())

        @pl.when(c + d < cols)
        def _():
            left(c + d, t).wait_recv()
            pl.when(has_left)(lambda: left(c + d, t).start())

        if d == cols - 1 and t + 2 < TOKEN_CHUNKS:
            send_a(t + 2)

    def take_w(j):
        for g in range(1, groups):
            source = peer(-g)
            w_copy(source, j, partner, p_send.at[j, g]).wait_recv()
            w_copy(source, j, partner, p_send.at[j, g]).start()

    def take_partner(j):
        for g in range(groups):
            source = 2 * g + 1 - core
            w_copy(source, j, partner, p_send.at[j, 0]).wait_recv()

    def product(rows_t, j):
        total = jnp.dot(abuf[0, rows_t, :], wbuf[j, pl.ds(0, depth_a), :], preferred_element_type=jnp.float32)
        for block in range(1, cols):
            total += jnp.dot(abuf[block, rows_t, :], wbuf[j, pl.ds(block * depth_a, depth_a), :], preferred_element_type=jnp.float32)
        return total

    def partials(tiles):
        t0, j0 = tiles[0]
        wide = 1 + tiles[-1][1] - j0

        def one(n, carry):
            t, j = t0 + n // wide, j0 + lax.rem(n, wide)
            rows_t = pl.ds(pl.multiple_of(t * tt, tt), tt)
            ysend[j, rows_t, :] = product(rows_t, j)
            return carry

        def send(n, carry):
            y_copy(t0 + n // wide, j0 + lax.rem(n, wide)).start()
            return carry

        lax.fori_loop(0, len(tiles), one, 0)
        lax.fori_loop(0, len(tiles), send, 0)

    def finish(j):
        def one(t, carry):
            rows_t = pl.ds(pl.multiple_of(t * tt * 2, tt * 2), tt * 2)
            y_copy(2 * t, j - jh).wait_recv()
            y_copy(2 * t + 1, j - jh).wait_recv()
            o_ref[rows_t, (j - jh) * nc:(j - jh + 1) * nc] = (product(rows_t, j) + yrecv[j - jh, rows_t, :]).astype(o_ref.dtype)
            return carry

        lax.fori_loop(0, TOKEN_CHUNKS // 2, one, 0)

    def part(j, rows_t, start, count):
        columns = pl.ds(pl.multiple_of(lax.rem(start, depth_a), min(count, depth_a)), count)
        weights = wbuf[j, pl.ds(pl.multiple_of(start, count), count), :]
        return jnp.dot(abuf[start // depth_a, rows_t, columns], weights, preferred_element_type=jnp.float32)

    def each_rows(body):
        def one(t, carry):
            body(pl.ds(pl.multiple_of(t * tt * 2, tt * 2), tt * 2))
            return carry

        lax.fori_loop(0, TOKEN_CHUNKS // 2, one, 0)

    def take_own_rows():
        for h in range(cuts):
            w_copy(partner, last + h, partner, p_send.at[last + h, 0]).wait_recv()
        count = min(depth_w, depth_a)
        for n in range(depth_w // count):
            @each_rows
            def _(rows_t):
                total = part(last, rows_t, r * depth_w + n * count, count) + part(last, rows_t, partner * depth_w + n * count, count)
                early[rows_t, :] = total if n == 0 else early[rows_t, :] + total

    def finish_last():
        count = depth_w // cuts
        for t in range(TOKEN_CHUNKS):
            y_copy(t, jh - 1).wait_recv()
        for h in range(cuts):
            take_w(last + h)
            for g in range(1, groups):
                own, other = peer(-g), peer(-g) + 1 - 2 * core

                @each_rows
                def _(rows_t):
                    early[rows_t, :] += part(last, rows_t, own * depth_w + h * count, count)

                w_copy(other, last + h, partner, p_send.at[last + h, 0]).wait_recv()

                @each_rows
                def _(rows_t):
                    total = early[rows_t, :] + part(last, rows_t, other * depth_w + h * count, count)
                    if h < cuts - 1 or g < groups - 1:
                        early[rows_t, :] = total
                    else:
                        o_ref[rows_t, (jh - 1) * nc:jh * nc] = (total + yrecv[jh - 1, rows_t, :]).astype(o_ref.dtype)

    got_t, got_j, done_own, own_rows = 0, 0, jh, False
    for _, kind, first, second in schedule(TOKEN_CHUNKS, COLUMN_CHUNKS, cols):
        if kind == 0:
            take_a(first, second)
            if second == cols - 1:
                got_t = first + 1
                if got_j:
                    partials([(first, j) for j in range(min(got_j, jh))])
        else:
            if first == last - 1 and got_t == TOKEN_CHUNKS:
                take_own_rows()
                own_rows = True
            take_w(first)
            take_partner(first)
            got_j = first + 1
            if first < jh and got_t:
                partials([(t, first) for t in range(got_t)])
        while got_t == TOKEN_CHUNKS and done_own < got_j:
            finish(done_own)
            done_own += 1
    if not own_rows:
        take_own_rows()
    finish_last()

    for t in range(TOKEN_CHUNKS):
        for block in range(cols):
            @pl.when(has_right & (block <= c))
            def _():
                right(block, t).wait_send()

            @pl.when(has_left & (block >= c))
            def _():
                left(block, t).wait_send()

        for j in range(jh):
            y_copy(t, j).wait_send()
    for p in range(pieces):
        for g in range(groups):
            w_copy(r, p, partner, p_send.at[p, g]).wait_send()
            if g:
                w_copy(r, p, partner, w_send.at[p, g]).wait_send()


PIECES = 16
FILL = 6
FILL_BACK = 3
LEAD = 3
LAG_O = 1
LAG_Y = 2
LAG_X = 5
SPAN = 250.0


def pair_kernel(rows, cols, a_ref, w_ref, o_ref, abuf, wbuf, acc, part, ysend, yrecv, xsend, xrecv, loc_a, loc_w, a_recv, f_send, b_send, c_send, w_send, w_recv, y_send, y_recv, x_send, x_recv):
    r, c, l = lax.axis_index("row"), lax.axis_index("col"), lax.axis_index("layer")
    x, core = r // 2, lax.rem(r, 2)
    partner, peer = 2 * x + 1 - core, 2 * (1 - x) + core
    step, u, far = 1 - 2 * x, c + x * (cols - 1 - 2 * c), cols - 1
    own = core + x * (1 - 2 * core)
    tokens, depth = a_ref.shape
    half = w_ref.shape[1] // 2
    tt, nc = tokens // PIECES, wbuf.shape[3]
    tiles = half // nc

    def rows_at(t, side):
        at = 2 * t if side == 0 else 2 * lax.rem(t + PIECES - LEAD, PIECES) + 1
        return pl.ds(pl.multiple_of(at * tt, tt), tt)

    def rows_of(t):
        return pl.ds(pl.multiple_of(t * tt, tt), tt)

    def a_at(v, side, t):
        return abuf.at[v, rows_at(t, side), :]

    def a_all(v):
        return abuf.at[v, pl.ds(0, tokens), :]

    def own_a(t):
        return pltpu.make_async_copy(a_ref.at[rows_of(t), :], a_at(u - u // far, 0, t), loc_a)

    def own_w(j):
        side = 1 - l if j < tiles else l
        at = pl.multiple_of(side * half + (j % tiles) * nc, nc)
        return pltpu.make_async_copy(w_ref.at[:, pl.ds(at, nc)], wbuf.at[own, j], loc_w)

    def remote(source, target, sent, got, **device):
        return pltpu.make_async_remote_copy(source, target, sent, got, device_id=device)

    def w_all(slot):
        return remote(wbuf.at[slot], wbuf.at[slot], w_send, w_recv, row=partner)

    def ahead(v, side, t):
        return remote(a_at(v, side, t), a_at(v, side, t), f_send.at[v + 2 * side], a_recv.at[v + 3 * side, t], col=c + step)

    def back(v, side, t):
        return remote(a_at(v, side, t), a_at(v, side, t), b_send.at[v - 1 + 2 * side], a_recv.at[v + 3 * side, t], col=c - step)

    def across(t):
        to = 1 - u // far
        return remote(a_at(2, 0, t), a_at(to, 1, t), c_send, a_recv.at[to + 3, t], row=peer)

    def y_copy(t, side):
        at = rows_at(t, side)
        return remote(ysend.at[at, :], yrecv.at[at, :], y_send, y_recv.at[t, side], layer=1 - l)

    def x_copy(t):
        at = rows_of(t)
        return remote(xsend.at[at, :], xrecv.at[at, :], x_send, x_recv.at[t], row=peer)

    def take(v, side, t):
        ahead(v, side, t).wait_recv()

    def within(first, t, body):
        if isinstance(t, int):
            if first <= t < PIECES:
                body(t)
        else:
            pl.when((t >= first) & (t < PIECES))(lambda: body(t))

    for t in range(PIECES):
        own_a(t).start()

    has_next, has_last = u < far, u > 0
    barrier = pltpu.get_barrier_semaphore()

    def greet(device_id):
        pl.semaphore_signal(barrier, inc=1, device_id=device_id)

    greet({"row": partner})
    greet({"row": peer})
    greet({"layer": 1 - l})
    pl.when(has_next)(lambda: greet({"col": c + step}))
    pl.when(has_last)(lambda: greet({"col": c - step}))
    pl.semaphore_wait(barrier, 3 + has_next.astype(jnp.int32) + has_last.astype(jnp.int32))

    pltpu.make_async_copy(a_ref, a_all(u - u // far), loc_a).wait()

    def send_first(t):
        ahead(0, 0, t).start()

    def send_ahead(t):
        ahead(1, 0, t).start()

    def send_back(t):
        back(1, 0, t).start()

    def each(start, stop, body):
        def one(t, carry):
            body(t)
            return carry

        lax.fori_loop(start, stop, one, 0)

    @pl.when(u == 0)
    def _():
        each(0, 2, send_first)

    @pl.when(u == 1)
    def _():
        for t in range(FILL):
            send_ahead(t)
            if t < FILL_BACK:
                send_back(t)

    @pl.when(u == 2)
    def _():
        def both(t):
            across(t).start()
            back(2, 0, t).start()

        each(0, PIECES, both)

    @pl.when(u == far)
    def _():
        each(0, PIECES, lambda t: across(t).start())

    for j in range(2 * tiles):
        own_w(j).start()
    pltpu.make_async_copy(wbuf.at[1 - own], wbuf.at[own], loc_w).wait()
    w_all(own).start()

    def on(v, side):
        def body(t):
            take(v, side, t)
            ahead(v, side, t).start()

        return body

    def cross(t):
        take(2, 0, t)
        across(t).start()

    def pass_back(t):
        take(2, 0, t)
        back(2, 0, t).start()
        across(t).start()
        take(1, 1, t)
        back(1, 1, t).start()

    @pl.when(u == 0)
    def _():
        for t in range(4):
            on(0, 1)(t)
            if t >= 2:
                send_first(t)

    @pl.when(u == 1)
    def _():
        for t in range(3):
            pass_back(t)
        for t in range(2):
            on(0, 1)(t)

    @pl.when(u == 2)
    def _():
        for t in range(FILL):
            on(1, 0)(t)

    def gather(t):
        @pl.when(u == 0)
        def _():
            within(0, t + LEAD, cross)
            within(4, t + LEAD + 4, on(0, 1))
            within(4, t + 4, send_first)
            within(0, t + LEAD, lambda t: take(1, 1, t))
            within(0, t, lambda t: take(1, 0, t))

        @pl.when(u == 1)
        def _():
            within(3, t + LEAD + 3, pass_back)
            within(FILL_BACK, t + 3, send_back)
            within(2, t + LEAD + 2, on(0, 1))
            within(0, t + 2, on(0, 0))
            within(FILL, t + 2, send_ahead)

        @pl.when(u == 2)
        def _():
            within(0, t + LEAD, on(0, 1))
            within(0, t, on(0, 0))
            within(FILL, t, on(1, 0))
            within(0, t + LEAD, lambda t: take(1, 1, t))

        @pl.when(u == far)
        def _():
            within(0, t + LEAD, lambda t: take(0, 1, t))
            within(0, t + LEAD, lambda t: take(1, 1, t))
            within(0, t, lambda t: take(0, 0, t))
            within(0, t, lambda t: take(1, 0, t))

    def encode(ref, at, value):
        scale = jnp.maximum(1.01 * jnp.max(jnp.abs(value), axis=1, keepdims=True), 1e-30).astype(jnp.bfloat16)
        level = jnp.exp2(jnp.abs(value) * (SPAN / scale.astype(jnp.float32)) - SPAN / 2)
        ref[at, :half] = jnp.where(value < 0, -level, level).astype(jnp.bfloat16)
        ref[at, half:] = jnp.broadcast_to(scale, (value.shape[0], ref.shape[1] - half))

    def decode(ref, at):
        level = ref[at, :half].astype(jnp.float32)
        scale = ref[at, half:half + 1].astype(jnp.float32)
        share = jnp.log2(jnp.abs(level)) * (1 / SPAN) + 0.5
        return jnp.where(level < 0, -share, share) * scale

    def multiply(at, sends, between=None):
        first, second = abuf[0, at, :], abuf[1, at, :]

        def product(j):
            return jnp.dot(first, wbuf[0, j], preferred_element_type=jnp.float32) + jnp.dot(second, wbuf[1, j], preferred_element_type=jnp.float32)

        for j in range(tiles):
            part[:at.size, j * nc:(j + 1) * nc] = product(j)
        for t, side, start in sends:
            encode(ysend, rows_at(t, side), part[start:start + tt, :])
        for t, side, start in sends:
            y_copy(t, side).start()
        if between:
            between()
        for j in range(tiles):
            acc[at, j * nc:(j + 1) * nc] = product(tiles + j)

    def reduce_other(t):
        y_copy(t, 1).wait_recv()
        at = rows_at(t, 1)
        encode(xsend, rows_of(t), acc[at, :] + decode(yrecv, at))
        x_copy(t).start()

    def reduce_own(t):
        y_copy(t, 0).wait_recv()
        at = rows_at(t, 0)
        acc[at, :] += decode(yrecv, at)

    def finish(t):
        x_copy(t).wait_recv()
        o_ref[rows_of(t), :] = (acc[rows_at(t, 0), :] + decode(xrecv, rows_of(t))).astype(o_ref.dtype)

    def finish_own(t):
        within(0, t - LAG_Y, reduce_own)
        within(0, t - LAG_X, finish)

    def reduce(t):
        within(0, t + LEAD - 1 - LAG_O, reduce_other)
        finish_own(t)

    def early(t):
        gather(t)
        multiply(rows_at(t + LEAD, 1), [(t + LEAD, 1, 0)])
        reduce(t)

    def steady(t):
        gather(t)
        multiply(pl.ds(pl.multiple_of(2 * t * tt, 2 * tt), 2 * tt), [(t + LEAD, 1, tt), (t, 0, 0)])
        reduce(t)

    def late(t):
        gather(t)
        multiply(rows_at(t, 0), [(t, 0, 0)], lambda: within(0, t + LEAD - 1 - LAG_O, reduce_other))
        finish_own(t)

    w_all(1 - own).wait_recv()
    each(-LEAD, 0, early)
    each(0, PIECES - LEAD, steady)
    each(PIECES - LEAD, PIECES, late)
    each(PIECES, PIECES + LAG_X, finish_own)

    def sent(sem):
        remote(a_all(0), a_all(0), sem, a_recv.at[0, 0], row=peer).wait_send()

    @pl.when(has_next)
    def _():
        sent(f_send.at[0])
        sent(f_send.at[2])
        pl.when(has_last)(lambda: sent(f_send.at[1]))

    @pl.when(u == 1)
    def _():
        sent(b_send.at[0])
        sent(b_send.at[2])

    pl.when(has_last & has_next)(lambda: sent(b_send.at[1]))
    sent(c_send)
    remote(ysend, yrecv, y_send, y_recv.at[0, 0], layer=1 - l).wait_send()
    remote(xsend, xrecv, x_send, x_recv.at[0], row=peer).wait_send()
    w_all(own).wait_send()


def pair_call(rows, cols, attn_values, out_weight):
    tokens, depth = attn_values.shape
    width = out_weight.shape[1]
    half = width // 2
    nc = half // 4
    dma = pltpu.SemaphoreType.DMA
    return pl.pallas_call(
        functools.partial(pair_kernel, rows, cols),
        out_shape=jax.ShapeDtypeStruct((tokens, half), jnp.bfloat16),
        in_specs=[pl.BlockSpec(memory_space=pltpu.HBM)] * 2,
        out_specs=pl.BlockSpec(memory_space=pltpu.VMEM),
        scratch_shapes=[
            pltpu.VMEM((3, 2 * tokens, depth), jnp.bfloat16),
            pltpu.VMEM((2, width // nc, depth, nc), jnp.bfloat16),
            pltpu.VMEM((2 * tokens, half), jnp.float32),
            pltpu.VMEM((2 * tokens // PIECES, half), jnp.float32),
            pltpu.VMEM((2 * tokens, half + 128), jnp.bfloat16),
            pltpu.VMEM((2 * tokens, half + 128), jnp.bfloat16),
            pltpu.VMEM((tokens, half + 128), jnp.bfloat16),
            pltpu.VMEM((tokens, half + 128), jnp.bfloat16),
            dma,
            dma,
            dma((5, PIECES)),
            dma((3,)),
            dma((3,)),
            dma,
            dma,
            dma,
            dma,
            dma((PIECES, 2)),
            dma,
            dma((PIECES,)),
        ],
        compiler_params=pltpu.CompilerParams(collective_id=1, has_side_effects=True, vmem_limit_bytes=48 * 2**20),
    )(*(pltpu.with_memory_space_constraint(v, pltpu.HBM) for v in (attn_values, out_weight)))


def solution(mesh):
    rows, cols = mesh.shape["row"], mesh.shape["col"]

    def shards(attn_values, out_weight):
        if rows == cols == 4:
            return pair_call(rows, cols, attn_values, out_weight)
        tokens, depth_a = attn_values.shape
        depth_w, width = out_weight.shape
        nc, jh = width // COLUMN_CHUNKS, COLUMN_CHUNKS // 2
        pieces = COLUMN_CHUNKS - 1 + last_pieces(depth_w)
        dma = pltpu.SemaphoreType.DMA
        return pl.pallas_call(
            functools.partial(kernel, rows, cols),
            out_shape=jax.ShapeDtypeStruct((tokens, width // 2), jnp.bfloat16),
            in_specs=[pl.BlockSpec(memory_space=pltpu.HBM)] * 2,
            out_specs=pl.BlockSpec(memory_space=pltpu.VMEM),
            scratch_shapes=[
                pltpu.VMEM((cols, tokens, depth_a), jnp.bfloat16),
                pltpu.VMEM((COLUMN_CHUNKS, rows * depth_w, nc), jnp.bfloat16),
                pltpu.VMEM((jh, tokens, nc), jnp.float32),
                pltpu.VMEM((jh, tokens, nc), jnp.float32),
                pltpu.VMEM((tokens, nc), jnp.float32),
                dma((TOKEN_CHUNKS,)),
                dma((pieces,)),
                dma((TOKEN_CHUNKS, cols)),
                dma((TOKEN_CHUNKS, cols)),
                dma((TOKEN_CHUNKS, cols)),
                dma((pieces, rows)),
                dma((pieces, rows // 2)),
                dma((pieces, rows // 2)),
                dma((TOKEN_CHUNKS, jh)),
                dma((TOKEN_CHUNKS, jh)),
            ],
            compiler_params=pltpu.CompilerParams(collective_id=0, has_side_effects=True, vmem_limit_bytes=48 * 2**20),
        )(*(pltpu.with_memory_space_constraint(x, pltpu.HBM) for x in (attn_values, out_weight)))

    in_specs = (P("row", ("layer", "col")), P(("layer", "row"), "col"))
    out_specs = P("row", ("col", "layer"))
    return jax.shard_map(shards, mesh=mesh, in_specs=in_specs, out_specs=out_specs, check_vma=False)
```

```python
import functools

import jax
import jax.numpy as jnp
from jax import lax
from jax.experimental import pallas as pl
from jax.experimental.pallas import tpu as pltpu
from jax.sharding import PartitionSpec as P

TOKEN_CHUNKS = 4
COLUMN_CHUNKS = 8


def last_pieces(depth_w):
    return max(1, min(4, depth_w // 256))


def schedule(token_chunks, column_chunks, col_count):
    events = []
    for t in range(token_chunks):
        for d in range(1, col_count):
            at = (col_count - 1) * t + (1 if d == 1 else d + 1)
            events.append((at, 0, t, d))
    span = (col_count - 1) * token_chunks * 4 / 3
    for j in range(column_chunks - 1):
        events.append((span * (j + 1) / column_chunks, 1, j, 0))
    ordered, clock = [], 0
    for at, kind, first, second in sorted(events, key=lambda e: (e[1], e[2], e[3])):
        if kind == 0:
            clock = max(clock, at)
            at = clock
        ordered.append((at, kind, first, second))
    return sorted(ordered)


def kernel(rows, cols, a_ref, w_ref, o_ref, abuf, wbuf, ysend, yrecv, early, loc_a, loc_w, a_recv, a_right, a_left, w_recv, w_send, p_send, y_recv, y_send):
    r, c, l = lax.axis_index("row"), lax.axis_index("col"), lax.axis_index("layer")
    groups = rows // 2
    core, group = lax.rem(r, 2), r // 2
    partner = 2 * group + 1 - core
    tokens, depth_a = a_ref.shape
    depth_w, width = w_ref.shape
    tt, half = tokens // TOKEN_CHUNKS, width // 2
    nc, jh = width // COLUMN_CHUNKS, COLUMN_CHUNKS // 2
    last, cuts = COLUMN_CHUNKS - 1, last_pieces(depth_w)
    pieces = last + cuts

    def piece(p):
        return (p, 0, depth_w) if p < last else (last, (p - last) * depth_w // cuts, depth_w // cuts)

    def peer(g):
        return 2 * lax.rem(group + g + groups, groups) + core

    def a_at(block, t):
        return abuf.at[block, pl.ds(t * tt, tt), :]

    def w_at(row, p):
        j, start, count = piece(p)
        return wbuf.at[j, pl.ds(pl.multiple_of(row * depth_w + start, count), count), :]

    def own_a(t):
        return pltpu.make_async_copy(a_ref.at[pl.ds(t * tt, tt), :], a_at(c, t), loc_a.at[t])

    def own_w(p):
        j, start, count = piece(p)
        side = 1 - l if j < jh else l
        at = pl.multiple_of(side * half + (j % jh) * nc, nc)
        return pltpu.make_async_copy(w_ref.at[pl.ds(start, count), pl.ds(at, nc)], w_at(r, p), loc_w.at[p])

    def a_copy(block, t, to, sems):
        return pltpu.make_async_remote_copy(a_at(block, t), a_at(block, t), sems.at[t, block], a_recv.at[t, block], device_id={"col": to})

    def w_copy(row, j, to, sem):
        return pltpu.make_async_remote_copy(w_at(row, j), w_at(row, j), sem, w_recv.at[j, row], device_id={"row": to})

    def y_copy(t, j):
        rows_t = pl.ds(t * tt, tt)
        return pltpu.make_async_remote_copy(ysend.at[j, rows_t, :], yrecv.at[j, rows_t, :], y_send.at[t, j], y_recv.at[t, j], device_id={"layer": 1 - l})

    def right(block, t):
        return a_copy(block, t, c + 1, a_right)

    def left(block, t):
        return a_copy(block, t, c - 1, a_left)

    for n in range(max(TOKEN_CHUNKS, pieces)):
        if n < pieces:
            own_w(n).start()
        if n < TOKEN_CHUNKS:
            own_a(n).start()

    has_right, has_left = c < cols - 1, c > 0
    barrier = pltpu.get_barrier_semaphore()

    def greet(device_id):
        pl.semaphore_signal(barrier, inc=1, device_id=device_id)

    greet({"row": partner})
    greet({"layer": 1 - l})
    for g in range(1, groups):
        greet({"row": peer(g)})
    pl.when(has_right)(lambda: greet({"col": c + 1}))
    pl.when(has_left)(lambda: greet({"col": c - 1}))
    pl.semaphore_wait(barrier, 1 + groups + has_right.astype(jnp.int32) + has_left.astype(jnp.int32))

    def send_a(t):
        own_a(t).wait()
        pl.when(has_right)(lambda: right(c, t).start())
        pl.when(has_left)(lambda: left(c, t).start())

    def send_w(j):
        own_w(j).wait()
        for g in range(1, groups):
            w_copy(r, j, peer(g), w_send.at[j, g]).start()
        w_copy(r, j, partner, p_send.at[j, 0]).start()

    send_w(0)
    send_a(0)
    send_a(1)
    for p in range(1, pieces):
        send_w(p)

    def take_a(t, d):
        @pl.when(c >= d)
        def _():
            right(c - d, t).wait_recv()
            pl.when(has_right)(lambda: right(c - d, t).start())

        @pl.when(c + d < cols)
        def _():
            left(c + d, t).wait_recv()
            pl.when(has_left)(lambda: left(c + d, t).start())

        if d == cols - 1 and t + 2 < TOKEN_CHUNKS:
            send_a(t + 2)

    def take_w(j):
        for g in range(1, groups):
            source = peer(-g)
            w_copy(source, j, partner, p_send.at[j, g]).wait_recv()
            w_copy(source, j, partner, p_send.at[j, g]).start()

    def take_partner(j):
        for g in range(groups):
            source = 2 * g + 1 - core
            w_copy(source, j, partner, p_send.at[j, 0]).wait_recv()

    def product(rows_t, j):
        total = jnp.dot(abuf[0, rows_t, :], wbuf[j, pl.ds(0, depth_a), :], preferred_element_type=jnp.float32)
        for block in range(1, cols):
            total += jnp.dot(abuf[block, rows_t, :], wbuf[j, pl.ds(block * depth_a, depth_a), :], preferred_element_type=jnp.float32)
        return total

    def partials(tiles):
        t0, j0 = tiles[0]
        wide = 1 + tiles[-1][1] - j0

        def one(n, carry):
            t, j = t0 + n // wide, j0 + lax.rem(n, wide)
            rows_t = pl.ds(pl.multiple_of(t * tt, tt), tt)
            ysend[j, rows_t, :] = product(rows_t, j)
            return carry

        def send(n, carry):
            y_copy(t0 + n // wide, j0 + lax.rem(n, wide)).start()
            return carry

        lax.fori_loop(0, len(tiles), one, 0)
        lax.fori_loop(0, len(tiles), send, 0)

    def finish(j):
        def one(t, carry):
            rows_t = pl.ds(pl.multiple_of(t * tt * 2, tt * 2), tt * 2)
            y_copy(2 * t, j - jh).wait_recv()
            y_copy(2 * t + 1, j - jh).wait_recv()
            o_ref[rows_t, (j - jh) * nc:(j - jh + 1) * nc] = (product(rows_t, j) + yrecv[j - jh, rows_t, :]).astype(o_ref.dtype)
            return carry

        lax.fori_loop(0, TOKEN_CHUNKS // 2, one, 0)

    def part(j, rows_t, start, count):
        columns = pl.ds(pl.multiple_of(lax.rem(start, depth_a), min(count, depth_a)), count)
        weights = wbuf[j, pl.ds(pl.multiple_of(start, count), count), :]
        return jnp.dot(abuf[start // depth_a, rows_t, columns], weights, preferred_element_type=jnp.float32)

    def each_rows(body):
        def one(t, carry):
            body(pl.ds(pl.multiple_of(t * tt * 2, tt * 2), tt * 2))
            return carry

        lax.fori_loop(0, TOKEN_CHUNKS // 2, one, 0)

    def take_own_rows():
        for h in range(cuts):
            w_copy(partner, last + h, partner, p_send.at[last + h, 0]).wait_recv()
        count = min(depth_w, depth_a)
        for n in range(depth_w // count):
            @each_rows
            def _(rows_t):
                total = part(last, rows_t, r * depth_w + n * count, count) + part(last, rows_t, partner * depth_w + n * count, count)
                early[rows_t, :] = total if n == 0 else early[rows_t, :] + total

    def finish_last():
        count = depth_w // cuts
        for t in range(TOKEN_CHUNKS):
            y_copy(t, jh - 1).wait_recv()
        for h in range(cuts):
            take_w(last + h)
            for g in range(1, groups):
                own, other = peer(-g), peer(-g) + 1 - 2 * core

                @each_rows
                def _(rows_t):
                    early[rows_t, :] += part(last, rows_t, own * depth_w + h * count, count)

                w_copy(other, last + h, partner, p_send.at[last + h, 0]).wait_recv()

                @each_rows
                def _(rows_t):
                    total = early[rows_t, :] + part(last, rows_t, other * depth_w + h * count, count)
                    if h < cuts - 1 or g < groups - 1:
                        early[rows_t, :] = total
                    else:
                        o_ref[rows_t, (jh - 1) * nc:jh * nc] = (total + yrecv[jh - 1, rows_t, :]).astype(o_ref.dtype)

    got_t, got_j, done_own, own_rows = 0, 0, jh, False
    for _, kind, first, second in schedule(TOKEN_CHUNKS, COLUMN_CHUNKS, cols):
        if kind == 0:
            take_a(first, second)
            if second == cols - 1:
                got_t = first + 1
                if got_j:
                    partials([(first, j) for j in range(min(got_j, jh))])
        else:
            if first == last - 1 and got_t == TOKEN_CHUNKS:
                take_own_rows()
                own_rows = True
            take_w(first)
            take_partner(first)
            got_j = first + 1
            if first < jh and got_t:
                partials([(t, first) for t in range(got_t)])
        while got_t == TOKEN_CHUNKS and done_own < got_j:
            finish(done_own)
            done_own += 1
    if not own_rows:
        take_own_rows()
    finish_last()

    for t in range(TOKEN_CHUNKS):
        for block in range(cols):
            @pl.when(has_right & (block <= c))
            def _():
                right(block, t).wait_send()

            @pl.when(has_left & (block >= c))
            def _():
                left(block, t).wait_send()

        for j in range(jh):
            y_copy(t, j).wait_send()
    for p in range(pieces):
        for g in range(groups):
            w_copy(r, p, partner, p_send.at[p, g]).wait_send()
            if g:
                w_copy(r, p, partner, w_send.at[p, g]).wait_send()


PIECES = 16
DETOURS = ((12, 2, 5), (14, 4, 7))
SHORT = 2
FILL = 6
FILL_BACK = 3
LEAD = 3
LAG_O = 1
LAG_Y = 2
LAG_X = 5
SPAN = 250.0


def pair_kernel(rows, cols, a_ref, w_ref, o_ref, abuf, wbuf, acc, part, ysend, yrecv, xsend, xrecv, loc_a, loc_w, a_recv, f_send, b_send, c_send, w_send, w_recv, y_send, y_recv, x_send, x_recv):
    r, c, l = lax.axis_index("row"), lax.axis_index("col"), lax.axis_index("layer")
    x, core = r // 2, lax.rem(r, 2)
    partner, peer = 2 * x + 1 - core, 2 * (1 - x) + core
    step, u, far = 1 - 2 * x, c + x * (cols - 1 - 2 * c), cols - 1
    own = core + x * (1 - 2 * core)
    tokens, depth = a_ref.shape
    half = w_ref.shape[1] // 2
    tt, nc = tokens // PIECES, wbuf.shape[3]
    tiles = half // nc

    def rows_at(t, side):
        at = 2 * t if side == 0 else 2 * lax.rem(t + PIECES - LEAD, PIECES) + 1
        return pl.ds(pl.multiple_of(at * tt, tt), tt)

    def rows_of(t):
        return pl.ds(pl.multiple_of(t * tt, tt), tt)

    def a_at(v, side, t):
        return abuf.at[v, rows_at(t, side), :]

    def a_all(v):
        return abuf.at[v, pl.ds(0, tokens), :]

    def own_a(t):
        return pltpu.make_async_copy(a_ref.at[rows_of(t), :], a_at(u - u // far, 0, t), loc_a)

    def own_w(j):
        side = 1 - l if j < tiles else l
        at = pl.multiple_of(side * half + (j % tiles) * nc, nc)
        return pltpu.make_async_copy(w_ref.at[:, pl.ds(at, nc)], wbuf.at[own, j], loc_w)

    def remote(source, target, sent, got, **device):
        return pltpu.make_async_remote_copy(source, target, sent, got, device_id=device)

    def w_all(slot):
        return remote(wbuf.at[slot], wbuf.at[slot], w_send, w_recv, row=partner)

    def ahead(v, side, t):
        return remote(a_at(v, side, t), a_at(v, side, t), f_send.at[v + 2 * side], a_recv.at[v + 2 * side, t], col=c + step)

    def back(v, side, t):
        return remote(a_at(v, side, t), a_at(v, side, t), b_send.at[v - 1 + 2 * side], a_recv.at[u - 1 if v == 2 else v + 2 * side, t], col=c - step)

    def across(t):
        to = 1 - u // far
        return remote(a_at(2, 0, t), a_at(to, 1, t), c_send, a_recv.at[to + 2, t], row=peer)

    def slot(t):
        return t if t < SHORT else SHORT + [n for n, _, _ in DETOURS].index(t)

    def leave(t):
        return remote(a_at(2, 0, t), a_at(2, 1, t), b_send.at[3], a_recv.at[4, slot(t)], col=c - step)

    def enter(t):
        return remote(a_at(2, 0, t), a_at(2, 1, t), f_send.at[3], a_recv.at[4, slot(t)], col=c + step)

    def back_other(t):
        return remote(a_at(2, 1, t), a_at(2, 1, t), b_send.at[3], a_recv.at[4, slot(t)], col=c - step)

    def over(t):
        to = u // far
        return remote(a_at(2, 1, t), a_at(to, 1, t), c_send, a_recv.at[to + 2, t], row=peer)

    def y_copy(t, side):
        at = rows_at(t, side)
        return remote(ysend.at[at, :], yrecv.at[at, :], y_send, y_recv.at[t, side], layer=1 - l)

    def x_copy(t):
        at = rows_of(t)
        return remote(xsend.at[at, :], xrecv.at[at, :], x_send, x_recv.at[t], row=peer)

    def take(v, side, t):
        ahead(v, side, t).wait_recv()

    def take_away(t):
        remote(a_at(2, 0, t), a_at(2, 0, t), b_send.at[1], a_recv.at[u, t], col=c - step).wait_recv()

    def take_other(t):
        enter(t).wait_recv()

    def within(first, t, body):
        if isinstance(t, int):
            if first <= t < PIECES:
                body(t)
        else:
            pl.when((t >= first) & (t < PIECES))(lambda: body(t))

    for t in range(PIECES):
        own_a(t).start()

    has_next, has_last = u < far, u > 0
    barrier = pltpu.get_barrier_semaphore()

    def greet(device_id):
        pl.semaphore_signal(barrier, inc=1, device_id=device_id)

    greet({"row": partner})
    greet({"row": peer})
    greet({"layer": 1 - l})
    pl.when(has_next)(lambda: greet({"col": c + step}))
    pl.when(has_last)(lambda: greet({"col": c - step}))
    pl.semaphore_wait(barrier, 3 + has_next.astype(jnp.int32) + has_last.astype(jnp.int32))

    pltpu.make_async_copy(a_ref, a_all(u - u // far), loc_a).wait()

    def send_first(t):
        ahead(0, 0, t).start()

    def send_ahead(t):
        ahead(1, 0, t).start()

    def send_back(t):
        back(1, 0, t).start()

    def each(start, stop, body):
        def one(t, carry):
            body(t)
            return carry

        lax.fori_loop(start, stop, one, 0)

    @pl.when(u == 0)
    def _():
        each(0, 2, send_first)

    @pl.when(u == 1)
    def _():
        for t in range(FILL):
            send_ahead(t)
            if t < FILL_BACK:
                send_back(t)

    @pl.when(u == 2)
    def _():
        for t in range(SHORT):
            enter(t).start()

        def both(t):
            across(t).start()
            back(2, 0, t).start()

        each(0, PIECES, both)

    @pl.when(u == far)
    def _():
        for t, _, _ in DETOURS:
            leave(t).start()
        each(0, 4, lambda t: across(t).start())

    for j in range(2 * tiles):
        own_w(j).start()
    pltpu.make_async_copy(wbuf.at[1 - own], wbuf.at[own], loc_w).wait()
    w_all(own).start()

    def on(v, side):
        def body(t):
            take(v, side, t)
            ahead(v, side, t).start()

        return body

    def unless(t, skipped, body):
        if isinstance(t, int):
            if t not in skipped:
                body()
        elif skipped:
            pl.when(functools.reduce(jnp.logical_and, [t != n for n in skipped]))(body)
        else:
            body()

    def on_most(t):
        take(0, 1, t)
        unless(t, [n for n, _, _ in DETOURS], lambda: ahead(0, 1, t).start())

    def on_back(t):
        take_other(t)
        back_other(t).start()

    def cross(t):
        take_away(t)
        across(t).start()

    def pass_back(t):
        take_away(t)
        back(2, 0, t).start()
        across(t).start()
        take(1, 1, t)
        unless(t, list(range(SHORT)), lambda: back(1, 1, t).start())

    @pl.when(u == 0)
    def _():
        for t in range(4):
            on(0, 1)(t)
            if t >= 2:
                send_first(t)

    @pl.when(u == 1)
    def _():
        for t in range(3):
            pass_back(t)
        for t in range(2):
            on_most(t)

    @pl.when(u == 2)
    def _():
        for t in range(FILL):
            on(1, 0)(t)
        for t, _, _ in DETOURS:
            on_back(t)
        on_most(0)

    @pl.when(u == far)
    def _():
        for t in range(SHORT):
            take_other(t)
            over(t).start()
        each(4, PIECES, lambda t: across(t).start())

    def gather(t):
        @pl.when(u == 0)
        def _():
            for n, _, at in DETOURS:
                @pl.when(t == at)
                def _():
                    take_other(n)
                    over(n).start()

            within(0, t + LEAD, cross)
            within(4, t + LEAD + 4, on(0, 1))
            within(4, t + 4, send_first)
            within(0, t + LEAD, lambda t: take(1, 1, t))
            within(0, t, lambda t: take(1, 0, t))

        @pl.when(u == 1)
        def _():
            for n, at, _ in DETOURS:
                @pl.when(t == at)
                def _():
                    on_back(n)
                    over(n).start()

            within(3, t + LEAD + 3, pass_back)
            within(FILL_BACK, t + 3, send_back)
            within(2, t + LEAD + 2, on_most)
            within(0, t + 2, on(0, 0))
            within(FILL, t + 2, send_ahead)

        @pl.when(u == 2)
        def _():
            within(0, t, on(0, 0))
            within(FILL, t, on(1, 0))
            within(0, t + LEAD, lambda t: take(1, 1, t))

        @pl.when(u == far)
        def _():
            within(0, t + LEAD, lambda t: take(0, 1, t))
            within(0, t + LEAD, lambda t: take(1, 1, t))
            within(0, t, lambda t: take(0, 0, t))
            within(0, t, lambda t: take(1, 0, t))

    def halfway(t):
        pl.when(u == 2)(lambda: within(0, t + LEAD + 1, on_most))

    def encode(ref, at, value):
        scale = jnp.maximum(1.01 * jnp.max(jnp.abs(value), axis=1, keepdims=True), 1e-30).astype(jnp.bfloat16)
        level = jnp.exp2(jnp.abs(value) * (SPAN / scale.astype(jnp.float32)) - SPAN / 2)
        ref[at, :half] = jnp.where(value < 0, -level, level).astype(jnp.bfloat16)
        ref[at, half:] = jnp.broadcast_to(scale, (value.shape[0], ref.shape[1] - half))

    def decode(ref, at):
        level = ref[at, :half].astype(jnp.float32)
        scale = ref[at, half:half + 1].astype(jnp.float32)
        share = jnp.log2(jnp.abs(level)) * (1 / SPAN) + 0.5
        return jnp.where(level < 0, -share, share) * scale

    def multiply(at, sends, between=None):
        first, second = abuf[0, at, :], abuf[1, at, :]

        def product(j):
            return jnp.dot(first, wbuf[0, j], preferred_element_type=jnp.float32) + jnp.dot(second, wbuf[1, j], preferred_element_type=jnp.float32)

        for j in range(tiles):
            part[:at.size, j * nc:(j + 1) * nc] = product(j)
        for t, side, start in sends:
            encode(ysend, rows_at(t, side), part[start:start + tt, :])
        for t, side, start in sends:
            y_copy(t, side).start()
        if between:
            between()
        for j in range(tiles):
            acc[at, j * nc:(j + 1) * nc] = product(tiles + j)

    def reduce_other(t):
        y_copy(t, 1).wait_recv()
        at = rows_at(t, 1)
        encode(xsend, rows_of(t), acc[at, :] + decode(yrecv, at))
        x_copy(t).start()

    def reduce_own(t):
        y_copy(t, 0).wait_recv()
        at = rows_at(t, 0)
        acc[at, :] += decode(yrecv, at)

    def finish(t):
        x_copy(t).wait_recv()
        o_ref[rows_of(t), :] = (acc[rows_at(t, 0), :] + decode(xrecv, rows_of(t))).astype(o_ref.dtype)

    def finish_own(t):
        within(0, t - LAG_Y, reduce_own)
        within(0, t - LAG_X, finish)

    def reduce(t):
        within(0, t + LEAD - 1 - LAG_O, reduce_other)
        finish_own(t)

    def early(t):
        gather(t)
        multiply(rows_at(t + LEAD, 1), [(t + LEAD, 1, 0)], lambda: halfway(t))
        reduce(t)

    def steady(t):
        gather(t)
        multiply(pl.ds(pl.multiple_of(2 * t * tt, 2 * tt), 2 * tt), [(t + LEAD, 1, tt), (t, 0, 0)], lambda: halfway(t))
        reduce(t)

    def late(t):
        gather(t)
        multiply(rows_at(t, 0), [(t, 0, 0)], lambda: within(0, t + LEAD - 1 - LAG_O, reduce_other))
        finish_own(t)

    w_all(1 - own).wait_recv()
    each(-LEAD, 0, early)
    each(0, PIECES - LEAD, steady)
    each(PIECES - LEAD, PIECES - 2, late)
    gather(PIECES - 2)
    gather(PIECES - 1)
    multiply(pl.ds(2 * (PIECES - 2) * tt, 4 * tt), [(PIECES - 2, 0, 0), (PIECES - 1, 0, 2 * tt)], lambda: reduce_other(PIECES - 1))
    finish_own(PIECES - 2)
    finish_own(PIECES - 1)
    each(PIECES, PIECES + LAG_X, finish_own)

    def sent(sem):
        remote(a_all(0), a_all(0), sem, a_recv.at[0, 0], row=peer).wait_send()

    def sent_few(sem, count):
        if count:
            some = abuf.at[0, pl.ds(0, count * tt), :]
            remote(some, some, sem, a_recv.at[0, 0], row=peer).wait_send()

    few = len(DETOURS)

    @pl.when(u == 0)
    def _():
        sent(f_send.at[0])
        sent(f_send.at[2])
        sent_few(c_send, few)

    @pl.when(u == 1)
    def _():
        for n in range(2):
            sent(f_send.at[n])
            sent(b_send.at[n])
        sent_few(f_send.at[2], PIECES - few)
        sent_few(b_send.at[2], PIECES - SHORT)
        sent_few(b_send.at[3], few)
        sent_few(c_send, few)

    @pl.when(u == 2)
    def _():
        for n in range(2):
            sent(f_send.at[n])
        sent(b_send.at[1])
        sent_few(f_send.at[2], PIECES - few)
        sent_few(f_send.at[3], SHORT)
        sent_few(b_send.at[3], few)

    @pl.when(u == far)
    def _():
        sent_few(b_send.at[3], few)
        sent_few(c_send, SHORT)

    sent(c_send)
    remote(ysend, yrecv, y_send, y_recv.at[0, 0], layer=1 - l).wait_send()
    remote(xsend, xrecv, x_send, x_recv.at[0], row=peer).wait_send()
    w_all(own).wait_send()


def pair_call(rows, cols, attn_values, out_weight):
    tokens, depth = attn_values.shape
    width = out_weight.shape[1]
    half = width // 2
    nc = half // 4
    dma = pltpu.SemaphoreType.DMA
    return pl.pallas_call(
        functools.partial(pair_kernel, rows, cols),
        out_shape=jax.ShapeDtypeStruct((tokens, half), jnp.bfloat16),
        in_specs=[pl.BlockSpec(memory_space=pltpu.HBM)] * 2,
        out_specs=pl.BlockSpec(memory_space=pltpu.VMEM),
        scratch_shapes=[
            pltpu.VMEM((3, 2 * tokens, depth), jnp.bfloat16),
            pltpu.VMEM((2, width // nc, depth, nc), jnp.bfloat16),
            pltpu.VMEM((2 * tokens, half), jnp.float32),
            pltpu.VMEM((4 * tokens // PIECES, half), jnp.float32),
            pltpu.VMEM((2 * tokens, half + 128), jnp.bfloat16),
            pltpu.VMEM((2 * tokens, half + 128), jnp.bfloat16),
            pltpu.VMEM((tokens, half + 128), jnp.bfloat16),
            pltpu.VMEM((tokens, half + 128), jnp.bfloat16),
            dma,
            dma,
            dma((5, PIECES)),
            dma((4,)),
            dma((4,)),
            dma,
            dma,
            dma,
            dma,
            dma((PIECES, 2)),
            dma,
            dma((PIECES,)),
        ],
        compiler_params=pltpu.CompilerParams(collective_id=1, has_side_effects=True, vmem_limit_bytes=48 * 2**20),
    )(*(pltpu.with_memory_space_constraint(v, pltpu.HBM) for v in (attn_values, out_weight)))


def solution(mesh):
    rows, cols = mesh.shape["row"], mesh.shape["col"]

    def shards(attn_values, out_weight):
        if rows == cols == 4:
            return pair_call(rows, cols, attn_values, out_weight)
        tokens, depth_a = attn_values.shape
        depth_w, width = out_weight.shape
        nc, jh = width // COLUMN_CHUNKS, COLUMN_CHUNKS // 2
        pieces = COLUMN_CHUNKS - 1 + last_pieces(depth_w)
        dma = pltpu.SemaphoreType.DMA
        return pl.pallas_call(
            functools.partial(kernel, rows, cols),
            out_shape=jax.ShapeDtypeStruct((tokens, width // 2), jnp.bfloat16),
            in_specs=[pl.BlockSpec(memory_space=pltpu.HBM)] * 2,
            out_specs=pl.BlockSpec(memory_space=pltpu.VMEM),
            scratch_shapes=[
                pltpu.VMEM((cols, tokens, depth_a), jnp.bfloat16),
                pltpu.VMEM((COLUMN_CHUNKS, rows * depth_w, nc), jnp.bfloat16),
                pltpu.VMEM((jh, tokens, nc), jnp.float32),
                pltpu.VMEM((jh, tokens, nc), jnp.float32),
                pltpu.VMEM((tokens, nc), jnp.float32),
                dma((TOKEN_CHUNKS,)),
                dma((pieces,)),
                dma((TOKEN_CHUNKS, cols)),
                dma((TOKEN_CHUNKS, cols)),
                dma((TOKEN_CHUNKS, cols)),
                dma((pieces, rows)),
                dma((pieces, rows // 2)),
                dma((pieces, rows // 2)),
                dma((TOKEN_CHUNKS, jh)),
                dma((TOKEN_CHUNKS, jh)),
            ],
            compiler_params=pltpu.CompilerParams(collective_id=0, has_side_effects=True, vmem_limit_bytes=48 * 2**20),
        )(*(pltpu.with_memory_space_constraint(x, pltpu.HBM) for x in (attn_values, out_weight)))

    in_specs = (P("row", ("layer", "col")), P(("layer", "row"), "col"))
    out_specs = P("row", ("col", "layer"))
    return jax.shard_map(shards, mesh=mesh, in_specs=in_specs, out_specs=out_specs, check_vma=False)
```

```python
import functools

import jax
import jax.numpy as jnp
from jax import lax
from jax.experimental import pallas as pl
from jax.experimental.pallas import tpu as pltpu
from jax.sharding import PartitionSpec as P

TOKEN_CHUNKS = 4
COLUMN_CHUNKS = 8


def last_pieces(depth_w):
    return max(1, min(4, depth_w // 256))


def schedule(token_chunks, column_chunks, col_count):
    events = []
    for t in range(token_chunks):
        for d in range(1, col_count):
            at = (col_count - 1) * t + (1 if d == 1 else d + 1)
            events.append((at, 0, t, d))
    span = (col_count - 1) * token_chunks * 4 / 3
    for j in range(column_chunks - 1):
        events.append((span * (j + 1) / column_chunks, 1, j, 0))
    ordered, clock = [], 0
    for at, kind, first, second in sorted(events, key=lambda e: (e[1], e[2], e[3])):
        if kind == 0:
            clock = max(clock, at)
            at = clock
        ordered.append((at, kind, first, second))
    return sorted(ordered)


def kernel(rows, cols, a_ref, w_ref, o_ref, abuf, wbuf, ysend, yrecv, early, loc_a, loc_w, a_recv, a_right, a_left, w_recv, w_send, p_send, y_recv, y_send):
    r, c, l = lax.axis_index("row"), lax.axis_index("col"), lax.axis_index("layer")
    groups = rows // 2
    core, group = lax.rem(r, 2), r // 2
    partner = 2 * group + 1 - core
    tokens, depth_a = a_ref.shape
    depth_w, width = w_ref.shape
    tt, half = tokens // TOKEN_CHUNKS, width // 2
    nc, jh = width // COLUMN_CHUNKS, COLUMN_CHUNKS // 2
    last, cuts = COLUMN_CHUNKS - 1, last_pieces(depth_w)
    pieces = last + cuts

    def piece(p):
        return (p, 0, depth_w) if p < last else (last, (p - last) * depth_w // cuts, depth_w // cuts)

    def peer(g):
        return 2 * lax.rem(group + g + groups, groups) + core

    def a_at(block, t):
        return abuf.at[block, pl.ds(t * tt, tt), :]

    def w_at(row, p):
        j, start, count = piece(p)
        return wbuf.at[j, pl.ds(pl.multiple_of(row * depth_w + start, count), count), :]

    def own_a(t):
        return pltpu.make_async_copy(a_ref.at[pl.ds(t * tt, tt), :], a_at(c, t), loc_a.at[t])

    def own_w(p):
        j, start, count = piece(p)
        side = 1 - l if j < jh else l
        at = pl.multiple_of(side * half + (j % jh) * nc, nc)
        return pltpu.make_async_copy(w_ref.at[pl.ds(start, count), pl.ds(at, nc)], w_at(r, p), loc_w.at[p])

    def a_copy(block, t, to, sems):
        return pltpu.make_async_remote_copy(a_at(block, t), a_at(block, t), sems.at[t, block], a_recv.at[t, block], device_id={"col": to})

    def w_copy(row, j, to, sem):
        return pltpu.make_async_remote_copy(w_at(row, j), w_at(row, j), sem, w_recv.at[j, row], device_id={"row": to})

    def y_copy(t, j):
        rows_t = pl.ds(t * tt, tt)
        return pltpu.make_async_remote_copy(ysend.at[j, rows_t, :], yrecv.at[j, rows_t, :], y_send.at[t, j], y_recv.at[t, j], device_id={"layer": 1 - l})

    def right(block, t):
        return a_copy(block, t, c + 1, a_right)

    def left(block, t):
        return a_copy(block, t, c - 1, a_left)

    for n in range(max(TOKEN_CHUNKS, pieces)):
        if n < pieces:
            own_w(n).start()
        if n < TOKEN_CHUNKS:
            own_a(n).start()

    has_right, has_left = c < cols - 1, c > 0
    barrier = pltpu.get_barrier_semaphore()

    def greet(device_id):
        pl.semaphore_signal(barrier, inc=1, device_id=device_id)

    greet({"row": partner})
    greet({"layer": 1 - l})
    for g in range(1, groups):
        greet({"row": peer(g)})
    pl.when(has_right)(lambda: greet({"col": c + 1}))
    pl.when(has_left)(lambda: greet({"col": c - 1}))
    pl.semaphore_wait(barrier, 1 + groups + has_right.astype(jnp.int32) + has_left.astype(jnp.int32))

    def send_a(t):
        own_a(t).wait()
        pl.when(has_right)(lambda: right(c, t).start())
        pl.when(has_left)(lambda: left(c, t).start())

    def send_w(j):
        own_w(j).wait()
        for g in range(1, groups):
            w_copy(r, j, peer(g), w_send.at[j, g]).start()
        w_copy(r, j, partner, p_send.at[j, 0]).start()

    send_w(0)
    send_a(0)
    send_a(1)
    for p in range(1, pieces):
        send_w(p)

    def take_a(t, d):
        @pl.when(c >= d)
        def _():
            right(c - d, t).wait_recv()
            pl.when(has_right)(lambda: right(c - d, t).start())

        @pl.when(c + d < cols)
        def _():
            left(c + d, t).wait_recv()
            pl.when(has_left)(lambda: left(c + d, t).start())

        if d == cols - 1 and t + 2 < TOKEN_CHUNKS:
            send_a(t + 2)

    def take_w(j):
        for g in range(1, groups):
            source = peer(-g)
            w_copy(source, j, partner, p_send.at[j, g]).wait_recv()
            w_copy(source, j, partner, p_send.at[j, g]).start()

    def take_partner(j):
        for g in range(groups):
            source = 2 * g + 1 - core
            w_copy(source, j, partner, p_send.at[j, 0]).wait_recv()

    def product(rows_t, j):
        total = jnp.dot(abuf[0, rows_t, :], wbuf[j, pl.ds(0, depth_a), :], preferred_element_type=jnp.float32)
        for block in range(1, cols):
            total += jnp.dot(abuf[block, rows_t, :], wbuf[j, pl.ds(block * depth_a, depth_a), :], preferred_element_type=jnp.float32)
        return total

    def partials(tiles):
        t0, j0 = tiles[0]
        wide = 1 + tiles[-1][1] - j0

        def one(n, carry):
            t, j = t0 + n // wide, j0 + lax.rem(n, wide)
            rows_t = pl.ds(pl.multiple_of(t * tt, tt), tt)
            ysend[j, rows_t, :] = product(rows_t, j)
            return carry

        def send(n, carry):
            y_copy(t0 + n // wide, j0 + lax.rem(n, wide)).start()
            return carry

        lax.fori_loop(0, len(tiles), one, 0)
        lax.fori_loop(0, len(tiles), send, 0)

    def finish(j):
        def one(t, carry):
            rows_t = pl.ds(pl.multiple_of(t * tt * 2, tt * 2), tt * 2)
            y_copy(2 * t, j - jh).wait_recv()
            y_copy(2 * t + 1, j - jh).wait_recv()
            o_ref[rows_t, (j - jh) * nc:(j - jh + 1) * nc] = (product(rows_t, j) + yrecv[j - jh, rows_t, :]).astype(o_ref.dtype)
            return carry

        lax.fori_loop(0, TOKEN_CHUNKS // 2, one, 0)

    def part(j, rows_t, start, count):
        columns = pl.ds(pl.multiple_of(lax.rem(start, depth_a), min(count, depth_a)), count)
        weights = wbuf[j, pl.ds(pl.multiple_of(start, count), count), :]
        return jnp.dot(abuf[start // depth_a, rows_t, columns], weights, preferred_element_type=jnp.float32)

    def each_rows(body):
        def one(t, carry):
            body(pl.ds(pl.multiple_of(t * tt * 2, tt * 2), tt * 2))
            return carry

        lax.fori_loop(0, TOKEN_CHUNKS // 2, one, 0)

    def take_own_rows():
        for h in range(cuts):
            w_copy(partner, last + h, partner, p_send.at[last + h, 0]).wait_recv()
        count = min(depth_w, depth_a)
        for n in range(depth_w // count):
            @each_rows
            def _(rows_t):
                total = part(last, rows_t, r * depth_w + n * count, count) + part(last, rows_t, partner * depth_w + n * count, count)
                early[rows_t, :] = total if n == 0 else early[rows_t, :] + total

    def finish_last():
        count = depth_w // cuts
        for t in range(TOKEN_CHUNKS):
            y_copy(t, jh - 1).wait_recv()
        for h in range(cuts):
            take_w(last + h)
            for g in range(1, groups):
                own, other = peer(-g), peer(-g) + 1 - 2 * core

                @each_rows
                def _(rows_t):
                    early[rows_t, :] += part(last, rows_t, own * depth_w + h * count, count)

                w_copy(other, last + h, partner, p_send.at[last + h, 0]).wait_recv()

                @each_rows
                def _(rows_t):
                    total = early[rows_t, :] + part(last, rows_t, other * depth_w + h * count, count)
                    if h < cuts - 1 or g < groups - 1:
                        early[rows_t, :] = total
                    else:
                        o_ref[rows_t, (jh - 1) * nc:jh * nc] = (total + yrecv[jh - 1, rows_t, :]).astype(o_ref.dtype)

    got_t, got_j, done_own, own_rows = 0, 0, jh, False
    for _, kind, first, second in schedule(TOKEN_CHUNKS, COLUMN_CHUNKS, cols):
        if kind == 0:
            take_a(first, second)
            if second == cols - 1:
                got_t = first + 1
                if got_j:
                    partials([(first, j) for j in range(min(got_j, jh))])
        else:
            if first == last - 1 and got_t == TOKEN_CHUNKS:
                take_own_rows()
                own_rows = True
            take_w(first)
            take_partner(first)
            got_j = first + 1
            if first < jh and got_t:
                partials([(t, first) for t in range(got_t)])
        while got_t == TOKEN_CHUNKS and done_own < got_j:
            finish(done_own)
            done_own += 1
    if not own_rows:
        take_own_rows()
    finish_last()

    for t in range(TOKEN_CHUNKS):
        for block in range(cols):
            @pl.when(has_right & (block <= c))
            def _():
                right(block, t).wait_send()

            @pl.when(has_left & (block >= c))
            def _():
                left(block, t).wait_send()

        for j in range(jh):
            y_copy(t, j).wait_send()
    for p in range(pieces):
        for g in range(groups):
            w_copy(r, p, partner, p_send.at[p, g]).wait_send()
            if g:
                w_copy(r, p, partner, w_send.at[p, g]).wait_send()


PIECES = 16
DETOURS = ((12, 0, 6), (14, 1, 8))
SHORT = 2
FILL = 6
FILL_BACK = 3
LEAD = 3
LAG_O = 1
LAG_Y = 2
LAG_X = 5
SPAN = 250.0


def pair_kernel(rows, cols, a_ref, w_ref, o_ref, abuf, wbuf, acc, part, ysend, yrecv, xsend, xrecv, loc_a, loc_w, a_recv, f_send, b_send, c_send, w_send, w_recv, y_send, y_recv, x_send, x_recv):
    r, c, l = lax.axis_index("row"), lax.axis_index("col"), lax.axis_index("layer")
    x, core = r // 2, lax.rem(r, 2)
    partner, peer = 2 * x + 1 - core, 2 * (1 - x) + core
    step, u, far = 1 - 2 * x, c + x * (cols - 1 - 2 * c), cols - 1
    own = core + x * (1 - 2 * core)
    tokens, depth = a_ref.shape
    half = w_ref.shape[1] // 2
    tt, nc = tokens // PIECES, wbuf.shape[3]
    tiles = half // nc

    def rows_at(t, side):
        at = 2 * t if side == 0 else 2 * lax.rem(t + PIECES - LEAD, PIECES) + 1
        return pl.ds(pl.multiple_of(at * tt, tt), tt)

    def rows_of(t):
        return pl.ds(pl.multiple_of(t * tt, tt), tt)

    def a_at(v, side, t):
        return abuf.at[v, rows_at(t, side), :]

    def a_all(v):
        return abuf.at[v, pl.ds(0, tokens), :]

    def own_a(t):
        return pltpu.make_async_copy(a_ref.at[rows_of(t), :], a_at(u - u // far, 0, t), loc_a)

    def own_w(j):
        side = 1 - l if j < tiles else l
        at = pl.multiple_of(side * half + (j % tiles) * nc, nc)
        return pltpu.make_async_copy(w_ref.at[:, pl.ds(at, nc)], wbuf.at[own, j], loc_w)

    def remote(source, target, sent, got, **device):
        return pltpu.make_async_remote_copy(source, target, sent, got, device_id=device)

    def w_all(slot):
        return remote(wbuf.at[slot], wbuf.at[slot], w_send, w_recv, row=partner)

    def ahead(v, side, t):
        return remote(a_at(v, side, t), a_at(v, side, t), f_send.at[v + 2 * side], a_recv.at[v + 2 * side, t], col=c + step)

    def back(v, side, t):
        return remote(a_at(v, side, t), a_at(v, side, t), b_send.at[v - 1 + 2 * side], a_recv.at[u - 1 if v == 2 else v + 2 * side, t], col=c - step)

    def across(t):
        to = 1 - u // far
        return remote(a_at(2, 0, t), a_at(to, 1, t), c_send, a_recv.at[to + 2, t], row=peer)

    def slot(t):
        return t if t < SHORT else SHORT + [n for n, _, _ in DETOURS].index(t)

    def leave(t):
        return remote(a_at(2, 0, t), a_at(2, 1, t), b_send.at[3], a_recv.at[4, slot(t)], col=c - step)

    def enter(t):
        return remote(a_at(2, 0, t), a_at(2, 1, t), f_send.at[3], a_recv.at[4, slot(t)], col=c + step)

    def back_other(t):
        return remote(a_at(2, 1, t), a_at(2, 1, t), b_send.at[3], a_recv.at[4, slot(t)], col=c - step)

    def over(t):
        to = u // far
        return remote(a_at(2, 1, t), a_at(to, 1, t), c_send, a_recv.at[to + 2, t], row=peer)

    def y_copy(t, side):
        at = rows_at(t, side)
        return remote(ysend.at[at, :], yrecv.at[at, :], y_send, y_recv.at[t, side], layer=1 - l)

    def x_copy(t):
        at = rows_of(t)
        return remote(xsend.at[at, :], xrecv.at[at, :], x_send, x_recv.at[t], row=peer)

    def take(v, side, t):
        ahead(v, side, t).wait_recv()

    def take_away(t):
        remote(a_at(2, 0, t), a_at(2, 0, t), b_send.at[1], a_recv.at[u, t], col=c - step).wait_recv()

    def take_other(t):
        enter(t).wait_recv()

    def within(first, t, body):
        if isinstance(t, int):
            if first <= t < PIECES:
                body(t)
        else:
            pl.when((t >= first) & (t < PIECES))(lambda: body(t))

    for t in range(PIECES):
        own_a(t).start()

    has_next, has_last = u < far, u > 0
    barrier = pltpu.get_barrier_semaphore()

    def greet(device_id):
        pl.semaphore_signal(barrier, inc=1, device_id=device_id)

    greet({"row": partner})
    greet({"row": peer})
    greet({"layer": 1 - l})
    pl.when(has_next)(lambda: greet({"col": c + step}))
    pl.when(has_last)(lambda: greet({"col": c - step}))
    pl.semaphore_wait(barrier, 3 + has_next.astype(jnp.int32) + has_last.astype(jnp.int32))

    pltpu.make_async_copy(a_ref, a_all(u - u // far), loc_a).wait()

    def send_first(t):
        ahead(0, 0, t).start()

    def send_ahead(t):
        ahead(1, 0, t).start()

    def send_back(t):
        back(1, 0, t).start()

    def each(start, stop, body):
        def one(t, carry):
            body(t)
            return carry

        lax.fori_loop(start, stop, one, 0)

    def both(t):
        across(t).start()
        back(2, 0, t).start()

    @pl.when(u == 0)
    def _():
        each(0, 2, send_first)

    @pl.when(u == 1)
    def _():
        for t in range(FILL):
            send_ahead(t)
            if t < FILL_BACK:
                send_back(t)

    @pl.when(u == 2)
    def _():
        for t in range(SHORT):
            enter(t).start()

        each(0, FILL, both)

    @pl.when(u == far)
    def _():
        for t, _, _ in DETOURS:
            leave(t).start()
        each(0, 4, lambda t: across(t).start())

    for j in range(2 * tiles):
        own_w(j).start()
    pltpu.make_async_copy(wbuf.at[1 - own], wbuf.at[own], loc_w).wait()
    w_all(own).start()

    def on(v, side):
        def body(t):
            take(v, side, t)
            ahead(v, side, t).start()

        return body

    def unless(t, skipped, body):
        if isinstance(t, int):
            if t not in skipped:
                body()
        elif skipped:
            pl.when(functools.reduce(jnp.logical_and, [t != n for n in skipped]))(body)
        else:
            body()

    def on_most(t):
        take(0, 1, t)
        unless(t, [n for n, _, _ in DETOURS], lambda: ahead(0, 1, t).start())

    def on_back(t):
        take_other(t)
        back_other(t).start()

    def cross(t):
        take_away(t)
        across(t).start()

    def pass_back(t):
        take_away(t)
        back(2, 0, t).start()
        across(t).start()
        take(1, 1, t)
        unless(t, list(range(SHORT)), lambda: back(1, 1, t).start())

    @pl.when(u == 0)
    def _():
        for t in range(4):
            on(0, 1)(t)
            if t >= 2:
                send_first(t)

    @pl.when(u == 1)
    def _():
        for t in range(3):
            pass_back(t)
        for t in range(2):
            on_most(t)

    @pl.when(u == 2)
    def _():
        for t in range(FILL):
            on(1, 0)(t)
            if t == 1:
                for n, _, _ in DETOURS:
                    on_back(n)
                each(FILL, PIECES, both)
        on_most(0)

    @pl.when(u == far)
    def _():
        for t in range(SHORT):
            take_other(t)
            over(t).start()
        each(4, PIECES, lambda t: across(t).start())

    def gather(t):
        @pl.when(u == 0)
        def _():
            for n, _, at in DETOURS:
                @pl.when(t == at)
                def _():
                    take_other(n)
                    over(n).start()

            within(0, t + LEAD, cross)
            within(4, t + LEAD + 4, on(0, 1))
            within(4, t + 4, send_first)
            within(0, t + LEAD, lambda t: take(1, 1, t))
            within(0, t, lambda t: take(1, 0, t))

        @pl.when(u == 1)
        def _():
            for n, at, _ in DETOURS:
                @pl.when(t == at)
                def _():
                    on_back(n)
                    over(n).start()

            within(3, t + LEAD + 3, pass_back)
            within(FILL_BACK, t + 3, send_back)
            within(2, t + LEAD + 2, on_most)
            within(0, t + 2, on(0, 0))
            within(FILL, t + 2, send_ahead)

        @pl.when(u == 2)
        def _():
            within(0, t, on(0, 0))
            within(FILL, t, on(1, 0))
            within(0, t + LEAD, lambda t: take(1, 1, t))

        @pl.when(u == far)
        def _():
            within(0, t + LEAD, lambda t: take(0, 1, t))
            within(0, t + LEAD, lambda t: take(1, 1, t))
            within(0, t, lambda t: take(0, 0, t))
            within(0, t, lambda t: take(1, 0, t))

    def halfway(t):
        pl.when(u == 2)(lambda: within(0, t + LEAD + 1, on_most))

    def encode(ref, at, value):
        scale = jnp.maximum(1.01 * jnp.max(jnp.abs(value), axis=1, keepdims=True), 1e-30).astype(jnp.bfloat16)
        level = jnp.exp2(jnp.abs(value) * (SPAN / scale.astype(jnp.float32)) - SPAN / 2)
        ref[at, :half] = jnp.where(value < 0, -level, level).astype(jnp.bfloat16)
        ref[at, half:] = jnp.broadcast_to(scale, (value.shape[0], ref.shape[1] - half))

    def decode(ref, at):
        level = ref[at, :half].astype(jnp.float32)
        scale = ref[at, half:half + 1].astype(jnp.float32)
        share = jnp.log2(jnp.abs(level)) * (1 / SPAN) + 0.5
        return jnp.where(level < 0, -share, share) * scale

    def multiply(at, sends, between=None):
        first, second = abuf[0, at, :], abuf[1, at, :]

        def product(j):
            return jnp.dot(first, wbuf[0, j], preferred_element_type=jnp.float32) + jnp.dot(second, wbuf[1, j], preferred_element_type=jnp.float32)

        for j in range(tiles):
            part[:at.size, j * nc:(j + 1) * nc] = product(j)
        for t, side, start in sends:
            encode(ysend, rows_at(t, side), part[start:start + tt, :])
        for t, side, start in sends:
            y_copy(t, side).start()
        if between:
            between()
        for j in range(tiles):
            acc[at, j * nc:(j + 1) * nc] = product(tiles + j)

    def reduce_other(t):
        y_copy(t, 1).wait_recv()
        at = rows_at(t, 1)
        encode(xsend, rows_of(t), acc[at, :] + decode(yrecv, at))
        x_copy(t).start()

    def reduce_own(t):
        y_copy(t, 0).wait_recv()
        at = rows_at(t, 0)
        acc[at, :] += decode(yrecv, at)

    def finish(t):
        x_copy(t).wait_recv()
        o_ref[rows_of(t), :] = (acc[rows_at(t, 0), :] + decode(xrecv, rows_of(t))).astype(o_ref.dtype)

    def finish_own(t):
        within(0, t - LAG_Y, reduce_own)
        within(0, t - LAG_X, finish)

    def reduce(t):
        within(0, t + LEAD - 1 - LAG_O, reduce_other)
        finish_own(t)

    def early(t):
        gather(t)
        multiply(rows_at(t + LEAD, 1), [(t + LEAD, 1, 0)], lambda: halfway(t))
        reduce(t)

    def steady(t):
        gather(t)
        multiply(pl.ds(pl.multiple_of(2 * t * tt, 2 * tt), 2 * tt), [(t + LEAD, 1, tt), (t, 0, 0)], lambda: halfway(t))
        reduce(t)

    def late(t):
        gather(t)
        multiply(rows_at(t, 0), [(t, 0, 0)], lambda: within(0, t + LEAD - 1 - LAG_O, reduce_other))
        finish_own(t)

    w_all(1 - own).wait_recv()
    each(-LEAD, 0, early)
    each(0, PIECES - LEAD, steady)
    each(PIECES - LEAD, PIECES - 2, late)
    gather(PIECES - 2)
    gather(PIECES - 1)
    multiply(pl.ds(2 * (PIECES - 2) * tt, 4 * tt), [(PIECES - 2, 0, 0), (PIECES - 1, 0, 2 * tt)], lambda: reduce_other(PIECES - 1))
    finish_own(PIECES - 2)
    finish_own(PIECES - 1)
    each(PIECES, PIECES + LAG_X, finish_own)

    def sent(sem):
        remote(a_all(0), a_all(0), sem, a_recv.at[0, 0], row=peer).wait_send()

    def sent_few(sem, count):
        if count:
            some = abuf.at[0, pl.ds(0, count * tt), :]
            remote(some, some, sem, a_recv.at[0, 0], row=peer).wait_send()

    few = len(DETOURS)

    @pl.when(u == 0)
    def _():
        sent(f_send.at[0])
        sent(f_send.at[2])
        sent_few(c_send, few)

    @pl.when(u == 1)
    def _():
        for n in range(2):
            sent(f_send.at[n])
            sent(b_send.at[n])
        sent_few(f_send.at[2], PIECES - few)
        sent_few(b_send.at[2], PIECES - SHORT)
        sent_few(b_send.at[3], few)
        sent_few(c_send, few)

    @pl.when(u == 2)
    def _():
        for n in range(2):
            sent(f_send.at[n])
        sent(b_send.at[1])
        sent_few(f_send.at[2], PIECES - few)
        sent_few(f_send.at[3], SHORT)
        sent_few(b_send.at[3], few)

    @pl.when(u == far)
    def _():
        sent_few(b_send.at[3], few)
        sent_few(c_send, SHORT)

    sent(c_send)
    remote(ysend, yrecv, y_send, y_recv.at[0, 0], layer=1 - l).wait_send()
    remote(xsend, xrecv, x_send, x_recv.at[0], row=peer).wait_send()
    w_all(own).wait_send()


def pair_call(rows, cols, attn_values, out_weight):
    tokens, depth = attn_values.shape
    width = out_weight.shape[1]
    half = width // 2
    nc = half // 4
    dma = pltpu.SemaphoreType.DMA
    return pl.pallas_call(
        functools.partial(pair_kernel, rows, cols),
        out_shape=jax.ShapeDtypeStruct((tokens, half), jnp.bfloat16),
        in_specs=[pl.BlockSpec(memory_space=pltpu.HBM)] * 2,
        out_specs=pl.BlockSpec(memory_space=pltpu.VMEM),
        scratch_shapes=[
            pltpu.VMEM((3, 2 * tokens, depth), jnp.bfloat16),
            pltpu.VMEM((2, width // nc, depth, nc), jnp.bfloat16),
            pltpu.VMEM((2 * tokens, half), jnp.float32),
            pltpu.VMEM((4 * tokens // PIECES, half), jnp.float32),
            pltpu.VMEM((2 * tokens, half + 128), jnp.bfloat16),
            pltpu.VMEM((2 * tokens, half + 128), jnp.bfloat16),
            pltpu.VMEM((tokens, half + 128), jnp.bfloat16),
            pltpu.VMEM((tokens, half + 128), jnp.bfloat16),
            dma,
            dma,
            dma((5, PIECES)),
            dma((4,)),
            dma((4,)),
            dma,
            dma,
            dma,
            dma,
            dma((PIECES, 2)),
            dma,
            dma((PIECES,)),
        ],
        compiler_params=pltpu.CompilerParams(collective_id=1, has_side_effects=True, vmem_limit_bytes=48 * 2**20),
    )(*(pltpu.with_memory_space_constraint(v, pltpu.HBM) for v in (attn_values, out_weight)))


def solution(mesh):
    rows, cols = mesh.shape["row"], mesh.shape["col"]

    def shards(attn_values, out_weight):
        if rows == cols == 4:
            return pair_call(rows, cols, attn_values, out_weight)
        tokens, depth_a = attn_values.shape
        depth_w, width = out_weight.shape
        nc, jh = width // COLUMN_CHUNKS, COLUMN_CHUNKS // 2
        pieces = COLUMN_CHUNKS - 1 + last_pieces(depth_w)
        dma = pltpu.SemaphoreType.DMA
        return pl.pallas_call(
            functools.partial(kernel, rows, cols),
            out_shape=jax.ShapeDtypeStruct((tokens, width // 2), jnp.bfloat16),
            in_specs=[pl.BlockSpec(memory_space=pltpu.HBM)] * 2,
            out_specs=pl.BlockSpec(memory_space=pltpu.VMEM),
            scratch_shapes=[
                pltpu.VMEM((cols, tokens, depth_a), jnp.bfloat16),
                pltpu.VMEM((COLUMN_CHUNKS, rows * depth_w, nc), jnp.bfloat16),
                pltpu.VMEM((jh, tokens, nc), jnp.float32),
                pltpu.VMEM((jh, tokens, nc), jnp.float32),
                pltpu.VMEM((tokens, nc), jnp.float32),
                dma((TOKEN_CHUNKS,)),
                dma((pieces,)),
                dma((TOKEN_CHUNKS, cols)),
                dma((TOKEN_CHUNKS, cols)),
                dma((TOKEN_CHUNKS, cols)),
                dma((pieces, rows)),
                dma((pieces, rows // 2)),
                dma((pieces, rows // 2)),
                dma((TOKEN_CHUNKS, jh)),
                dma((TOKEN_CHUNKS, jh)),
            ],
            compiler_params=pltpu.CompilerParams(collective_id=0, has_side_effects=True, vmem_limit_bytes=48 * 2**20),
        )(*(pltpu.with_memory_space_constraint(x, pltpu.HBM) for x in (attn_values, out_weight)))

    in_specs = (P("row", ("layer", "col")), P(("layer", "row"), "col"))
    out_specs = P("row", ("col", "layer"))
    return jax.shard_map(shards, mesh=mesh, in_specs=in_specs, out_specs=out_specs, check_vma=False)
```

```python
import functools

import jax
import jax.numpy as jnp
from jax import lax
from jax.experimental import pallas as pl
from jax.experimental.pallas import tpu as pltpu
from jax.sharding import PartitionSpec as P

TOKEN_CHUNKS = 4
COLUMN_CHUNKS = 8


def last_pieces(depth_w):
    return max(1, min(4, depth_w // 256))


def schedule(token_chunks, column_chunks, col_count):
    events = []
    for t in range(token_chunks):
        for d in range(1, col_count):
            at = (col_count - 1) * t + (1 if d == 1 else d + 1)
            events.append((at, 0, t, d))
    span = (col_count - 1) * token_chunks * 4 / 3
    for j in range(column_chunks - 1):
        events.append((span * (j + 1) / column_chunks, 1, j, 0))
    ordered, clock = [], 0
    for at, kind, first, second in sorted(events, key=lambda e: (e[1], e[2], e[3])):
        if kind == 0:
            clock = max(clock, at)
            at = clock
        ordered.append((at, kind, first, second))
    return sorted(ordered)


def kernel(rows, cols, a_ref, w_ref, o_ref, abuf, wbuf, ysend, yrecv, early, loc_a, loc_w, a_recv, a_right, a_left, w_recv, w_send, p_send, y_recv, y_send):
    r, c, l = lax.axis_index("row"), lax.axis_index("col"), lax.axis_index("layer")
    groups = rows // 2
    core, group = lax.rem(r, 2), r // 2
    partner = 2 * group + 1 - core
    tokens, depth_a = a_ref.shape
    depth_w, width = w_ref.shape
    tt, half = tokens // TOKEN_CHUNKS, width // 2
    nc, jh = width // COLUMN_CHUNKS, COLUMN_CHUNKS // 2
    last, cuts = COLUMN_CHUNKS - 1, last_pieces(depth_w)
    pieces = last + cuts

    def piece(p):
        return (p, 0, depth_w) if p < last else (last, (p - last) * depth_w // cuts, depth_w // cuts)

    def peer(g):
        return 2 * lax.rem(group + g + groups, groups) + core

    def a_at(block, t):
        return abuf.at[block, pl.ds(t * tt, tt), :]

    def w_at(row, p):
        j, start, count = piece(p)
        return wbuf.at[j, pl.ds(pl.multiple_of(row * depth_w + start, count), count), :]

    def own_a(t):
        return pltpu.make_async_copy(a_ref.at[pl.ds(t * tt, tt), :], a_at(c, t), loc_a.at[t])

    def own_w(p):
        j, start, count = piece(p)
        side = 1 - l if j < jh else l
        at = pl.multiple_of(side * half + (j % jh) * nc, nc)
        return pltpu.make_async_copy(w_ref.at[pl.ds(start, count), pl.ds(at, nc)], w_at(r, p), loc_w.at[p])

    def a_copy(block, t, to, sems):
        return pltpu.make_async_remote_copy(a_at(block, t), a_at(block, t), sems.at[t, block], a_recv.at[t, block], device_id={"col": to})

    def w_copy(row, j, to, sem):
        return pltpu.make_async_remote_copy(w_at(row, j), w_at(row, j), sem, w_recv.at[j, row], device_id={"row": to})

    def y_copy(t, j):
        rows_t = pl.ds(t * tt, tt)
        return pltpu.make_async_remote_copy(ysend.at[j, rows_t, :], yrecv.at[j, rows_t, :], y_send.at[t, j], y_recv.at[t, j], device_id={"layer": 1 - l})

    def right(block, t):
        return a_copy(block, t, c + 1, a_right)

    def left(block, t):
        return a_copy(block, t, c - 1, a_left)

    for n in range(max(TOKEN_CHUNKS, pieces)):
        if n < pieces:
            own_w(n).start()
        if n < TOKEN_CHUNKS:
            own_a(n).start()

    has_right, has_left = c < cols - 1, c > 0
    barrier = pltpu.get_barrier_semaphore()

    def greet(device_id):
        pl.semaphore_signal(barrier, inc=1, device_id=device_id)

    greet({"row": partner})
    greet({"layer": 1 - l})
    for g in range(1, groups):
        greet({"row": peer(g)})
    pl.when(has_right)(lambda: greet({"col": c + 1}))
    pl.when(has_left)(lambda: greet({"col": c - 1}))
    pl.semaphore_wait(barrier, 1 + groups + has_right.astype(jnp.int32) + has_left.astype(jnp.int32))

    def send_a(t):
        own_a(t).wait()
        pl.when(has_right)(lambda: right(c, t).start())
        pl.when(has_left)(lambda: left(c, t).start())

    def send_w(j):
        own_w(j).wait()
        for g in range(1, groups):
            w_copy(r, j, peer(g), w_send.at[j, g]).start()
        w_copy(r, j, partner, p_send.at[j, 0]).start()

    send_w(0)
    send_a(0)
    send_a(1)
    for p in range(1, pieces):
        send_w(p)

    def take_a(t, d):
        @pl.when(c >= d)
        def _():
            right(c - d, t).wait_recv()
            pl.when(has_right)(lambda: right(c - d, t).start())

        @pl.when(c + d < cols)
        def _():
            left(c + d, t).wait_recv()
            pl.when(has_left)(lambda: left(c + d, t).start())

        if d == cols - 1 and t + 2 < TOKEN_CHUNKS:
            send_a(t + 2)

    def take_w(j):
        for g in range(1, groups):
            source = peer(-g)
            w_copy(source, j, partner, p_send.at[j, g]).wait_recv()
            w_copy(source, j, partner, p_send.at[j, g]).start()

    def take_partner(j):
        for g in range(groups):
            source = 2 * g + 1 - core
            w_copy(source, j, partner, p_send.at[j, 0]).wait_recv()

    def product(rows_t, j):
        total = jnp.dot(abuf[0, rows_t, :], wbuf[j, pl.ds(0, depth_a), :], preferred_element_type=jnp.float32)
        for block in range(1, cols):
            total += jnp.dot(abuf[block, rows_t, :], wbuf[j, pl.ds(block * depth_a, depth_a), :], preferred_element_type=jnp.float32)
        return total

    def partials(tiles):
        t0, j0 = tiles[0]
        wide = 1 + tiles[-1][1] - j0

        def one(n, carry):
            t, j = t0 + n // wide, j0 + lax.rem(n, wide)
            rows_t = pl.ds(pl.multiple_of(t * tt, tt), tt)
            ysend[j, rows_t, :] = product(rows_t, j)
            return carry

        def send(n, carry):
            y_copy(t0 + n // wide, j0 + lax.rem(n, wide)).start()
            return carry

        lax.fori_loop(0, len(tiles), one, 0)
        lax.fori_loop(0, len(tiles), send, 0)

    def finish(j):
        def one(t, carry):
            rows_t = pl.ds(pl.multiple_of(t * tt * 2, tt * 2), tt * 2)
            y_copy(2 * t, j - jh).wait_recv()
            y_copy(2 * t + 1, j - jh).wait_recv()
            o_ref[rows_t, (j - jh) * nc:(j - jh + 1) * nc] = (product(rows_t, j) + yrecv[j - jh, rows_t, :]).astype(o_ref.dtype)
            return carry

        lax.fori_loop(0, TOKEN_CHUNKS // 2, one, 0)

    def part(j, rows_t, start, count):
        columns = pl.ds(pl.multiple_of(lax.rem(start, depth_a), min(count, depth_a)), count)
        weights = wbuf[j, pl.ds(pl.multiple_of(start, count), count), :]
        return jnp.dot(abuf[start // depth_a, rows_t, columns], weights, preferred_element_type=jnp.float32)

    def each_rows(body):
        def one(t, carry):
            body(pl.ds(pl.multiple_of(t * tt * 2, tt * 2), tt * 2))
            return carry

        lax.fori_loop(0, TOKEN_CHUNKS // 2, one, 0)

    def take_own_rows():
        for h in range(cuts):
            w_copy(partner, last + h, partner, p_send.at[last + h, 0]).wait_recv()
        count = min(depth_w, depth_a)
        for n in range(depth_w // count):
            @each_rows
            def _(rows_t):
                total = part(last, rows_t, r * depth_w + n * count, count) + part(last, rows_t, partner * depth_w + n * count, count)
                early[rows_t, :] = total if n == 0 else early[rows_t, :] + total

    def finish_last():
        count = depth_w // cuts
        for t in range(TOKEN_CHUNKS):
            y_copy(t, jh - 1).wait_recv()
        for h in range(cuts):
            take_w(last + h)
            for g in range(1, groups):
                own, other = peer(-g), peer(-g) + 1 - 2 * core

                @each_rows
                def _(rows_t):
                    early[rows_t, :] += part(last, rows_t, own * depth_w + h * count, count)

                w_copy(other, last + h, partner, p_send.at[last + h, 0]).wait_recv()

                @each_rows
                def _(rows_t):
                    total = early[rows_t, :] + part(last, rows_t, other * depth_w + h * count, count)
                    if h < cuts - 1 or g < groups - 1:
                        early[rows_t, :] = total
                    else:
                        o_ref[rows_t, (jh - 1) * nc:jh * nc] = (total + yrecv[jh - 1, rows_t, :]).astype(o_ref.dtype)

    got_t, got_j, done_own, own_rows = 0, 0, jh, False
    for _, kind, first, second in schedule(TOKEN_CHUNKS, COLUMN_CHUNKS, cols):
        if kind == 0:
            take_a(first, second)
            if second == cols - 1:
                got_t = first + 1
                if got_j:
                    partials([(first, j) for j in range(min(got_j, jh))])
        else:
            if first == last - 1 and got_t == TOKEN_CHUNKS:
                take_own_rows()
                own_rows = True
            take_w(first)
            take_partner(first)
            got_j = first + 1
            if first < jh and got_t:
                partials([(t, first) for t in range(got_t)])
        while got_t == TOKEN_CHUNKS and done_own < got_j:
            finish(done_own)
            done_own += 1
    if not own_rows:
        take_own_rows()
    finish_last()

    for t in range(TOKEN_CHUNKS):
        for block in range(cols):
            @pl.when(has_right & (block <= c))
            def _():
                right(block, t).wait_send()

            @pl.when(has_left & (block >= c))
            def _():
                left(block, t).wait_send()

        for j in range(jh):
            y_copy(t, j).wait_send()
    for p in range(pieces):
        for g in range(groups):
            w_copy(r, p, partner, p_send.at[p, g]).wait_send()
            if g:
                w_copy(r, p, partner, w_send.at[p, g]).wait_send()


PIECES = 16
DETOURS = ((12, 0, 6), (14, 1, 8))
SHORT = 2
FILL = 6
FILL_BACK = 3
LEAD = 3
LAG_O = 1
LAG_Y = 2
LAG_X = 5
SPAN = 250.0


def pair_kernel(rows, cols, a_ref, w_ref, o_ref, abuf, wbuf, acc, part, ysend, yrecv, xsend, xrecv, loc_a, loc_w, a_recv, o_recv, f_send, b_send, c_send, w_send, w_recv, y_send, y_recv, x_send, x_recv):
    r, c, l = lax.axis_index("row"), lax.axis_index("col"), lax.axis_index("layer")
    x, core = r // 2, lax.rem(r, 2)
    partner, peer = 2 * x + 1 - core, 2 * (1 - x) + core
    step, u, far = 1 - 2 * x, c + x * (cols - 1 - 2 * c), cols - 1
    own = core + x * (1 - 2 * core)
    tokens, depth = a_ref.shape
    half = w_ref.shape[1] // 2
    tt, nc = tokens // PIECES, wbuf.shape[3]
    tiles = half // nc

    def rows_at(t, side):
        at = 2 * t if side == 0 else 2 * lax.rem(t + PIECES - LEAD, PIECES) + 1
        return pl.ds(pl.multiple_of(at * tt, tt), tt)

    def rows_of(t):
        return pl.ds(pl.multiple_of(t * tt, tt), tt)

    def a_at(v, side, t):
        return abuf.at[v, rows_at(t, side), :]

    def a_all(v):
        return abuf.at[v, pl.ds(0, tokens), :]

    def own_a(t):
        return pltpu.make_async_copy(a_ref.at[rows_of(t), :], a_at(u - u // far, 0, t), loc_a)

    def own_w(j):
        side = 1 - l if j < tiles else l
        at = pl.multiple_of(side * half + (j % tiles) * nc, nc)
        return pltpu.make_async_copy(w_ref.at[:, pl.ds(at, nc)], wbuf.at[own, j], loc_w)

    def remote(source, target, sent, got, **device):
        return pltpu.make_async_remote_copy(source, target, sent, got, device_id=device)

    def w_all(slot):
        return remote(wbuf.at[slot], wbuf.at[slot], w_send, w_recv, row=partner)

    def ahead(v, side, t):
        return remote(a_at(v, side, t), a_at(v, side, t), f_send.at[v + 2 * side], a_recv.at[v + 2 * side, t], col=c + step)

    def back(v, side, t):
        return remote(a_at(v, side, t), a_at(v, side, t), b_send.at[v - 1 + 2 * side], a_recv.at[u - 1 if v == 2 else v + 2 * side, t], col=c - step)

    def across(t):
        to = 1 - u // far
        return remote(a_at(2, 0, t), a_at(to, 1, t), c_send, a_recv.at[to + 2, t], row=peer)

    def slot(t):
        return t if t < SHORT else SHORT + [n for n, _, _ in DETOURS].index(t)

    def leave(t):
        return remote(a_at(2, 0, t), a_at(2, 1, t), b_send.at[3], o_recv.at[slot(t)], col=c - step)

    def enter(t):
        return remote(a_at(2, 0, t), a_at(2, 1, t), f_send.at[3], o_recv.at[slot(t)], col=c + step)

    def back_other(t):
        return remote(a_at(2, 1, t), a_at(2, 1, t), b_send.at[3], o_recv.at[slot(t)], col=c - step)

    def over(t):
        to = u // far
        return remote(a_at(2, 1, t), a_at(to, 1, t), c_send, a_recv.at[to + 2, t], row=peer)

    def y_copy(t, side):
        at = rows_at(t, side)
        return remote(ysend.at[at, :], yrecv.at[at, :], y_send, y_recv.at[t, side], layer=1 - l)

    def x_copy(t):
        at = rows_of(t)
        return remote(xsend.at[at, :], xrecv.at[at, :], x_send, x_recv.at[t], row=peer)

    def take(v, side, t):
        ahead(v, side, t).wait_recv()

    def take_away(t):
        remote(a_at(2, 0, t), a_at(2, 0, t), b_send.at[1], a_recv.at[u, t], col=c - step).wait_recv()

    def take_other(t):
        enter(t).wait_recv()

    def within(first, t, body):
        if isinstance(t, int):
            if first <= t < PIECES:
                body(t)
        else:
            pl.when((t >= first) & (t < PIECES))(lambda: body(t))

    for t in range(PIECES):
        own_a(t).start()

    has_next, has_last = u < far, u > 0
    barrier = pltpu.get_barrier_semaphore()

    def greet(device_id):
        pl.semaphore_signal(barrier, inc=1, device_id=device_id)

    greet({"row": partner})
    greet({"row": peer})
    greet({"layer": 1 - l})
    pl.when(has_next)(lambda: greet({"col": c + step}))
    pl.when(has_last)(lambda: greet({"col": c - step}))
    pl.semaphore_wait(barrier, 3 + has_next.astype(jnp.int32) + has_last.astype(jnp.int32))

    pltpu.make_async_copy(a_ref, a_all(u - u // far), loc_a).wait()

    def send_first(t):
        ahead(0, 0, t).start()

    def send_ahead(t):
        ahead(1, 0, t).start()

    def send_back(t):
        back(1, 0, t).start()

    def each(start, stop, body):
        def one(t, carry):
            body(t)
            return carry

        lax.fori_loop(start, stop, one, 0)

    def both(t):
        across(t).start()
        back(2, 0, t).start()

    @pl.when(u == 0)
    def _():
        each(0, 2, send_first)

    @pl.when(u == 1)
    def _():
        for t in range(FILL):
            send_ahead(t)
            if t < FILL_BACK:
                send_back(t)

    @pl.when(u == 2)
    def _():
        for t in range(SHORT):
            enter(t).start()

        each(0, FILL, both)

    @pl.when(u == far)
    def _():
        for t, _, _ in DETOURS:
            leave(t).start()
        each(0, 4, lambda t: across(t).start())

    for j in range(2 * tiles):
        own_w(j).start()
    pltpu.make_async_copy(wbuf.at[1 - own], wbuf.at[own], loc_w).wait()
    w_all(own).start()

    def on(v, side):
        def body(t):
            take(v, side, t)
            ahead(v, side, t).start()

        return body

    def unless(t, skipped, body):
        if isinstance(t, int):
            if t not in skipped:
                body()
        elif skipped:
            pl.when(functools.reduce(jnp.logical_and, [t != n for n in skipped]))(body)
        else:
            body()

    def on_most(t):
        take(0, 1, t)
        unless(t, [n for n, _, _ in DETOURS], lambda: ahead(0, 1, t).start())

    def on_back(t):
        take_other(t)
        back_other(t).start()

    def cross(t):
        take_away(t)
        across(t).start()

    def pass_back(t):
        take_away(t)
        back(2, 0, t).start()
        across(t).start()
        take(1, 1, t)
        unless(t, list(range(SHORT)), lambda: back(1, 1, t).start())

    @pl.when(u == 0)
    def _():
        for t in range(4):
            on(0, 1)(t)
            if t >= 2:
                send_first(t)

    @pl.when(u == 1)
    def _():
        for t in range(3):
            pass_back(t)
        for t in range(2):
            on_most(t)

    @pl.when(u == 2)
    def _():
        for t in range(FILL):
            on(1, 0)(t)
            if t == 1:
                for n, _, _ in DETOURS:
                    on_back(n)
                each(FILL, PIECES, both)
        on_most(0)

    @pl.when(u == far)
    def _():
        for t in range(SHORT):
            take_other(t)
            over(t).start()
        each(4, PIECES, lambda t: across(t).start())

    def gather(t):
        @pl.when(u == 0)
        def _():
            for n, _, at in DETOURS:
                @pl.when(t == at)
                def _():
                    take_other(n)
                    over(n).start()

            within(0, t + LEAD, cross)
            within(4, t + LEAD + 4, on(0, 1))
            within(4, t + 4, send_first)
            within(0, t + LEAD, lambda t: take(1, 1, t))
            within(0, t, lambda t: take(1, 0, t))

        @pl.when(u == 1)
        def _():
            for n, at, _ in DETOURS:
                @pl.when(t == at)
                def _():
                    on_back(n)
                    over(n).start()

            within(3, t + LEAD + 3, pass_back)
            within(FILL_BACK, t + 3, send_back)
            within(2, t + LEAD + 2, on_most)
            within(0, t + 2, on(0, 0))
            within(FILL, t + 2, send_ahead)

        @pl.when(u == 2)
        def _():
            within(0, t, on(0, 0))
            within(FILL, t, on(1, 0))
            within(0, t + LEAD, lambda t: take(1, 1, t))

        @pl.when(u == far)
        def _():
            within(0, t + LEAD, lambda t: take(0, 1, t))
            within(0, t + LEAD, lambda t: take(1, 1, t))
            within(0, t, lambda t: take(0, 0, t))
            within(0, t, lambda t: take(1, 0, t))

    def halfway(t):
        pl.when(u == 2)(lambda: within(0, t + LEAD + 1, on_most))

    def encode(ref, at, value):
        scale = jnp.maximum(1.01 * jnp.max(jnp.abs(value), axis=1, keepdims=True), 1e-30).astype(jnp.bfloat16)
        level = jnp.exp2(jnp.abs(value) * (SPAN / scale.astype(jnp.float32)) - SPAN / 2)
        ref[at, :half] = jnp.where(value < 0, -level, level).astype(jnp.bfloat16)
        ref[at, half:] = jnp.broadcast_to(scale, (value.shape[0], ref.shape[1] - half))

    def decode(ref, at):
        level = ref[at, :half].astype(jnp.float32)
        scale = ref[at, half:half + 1].astype(jnp.float32)
        share = jnp.log2(jnp.abs(level)) * (1 / SPAN) + 0.5
        return jnp.where(level < 0, -share, share) * scale

    def multiply(at, sends, between=None):
        first, second = abuf[0, at, :], abuf[1, at, :]

        def product(j):
            return jnp.dot(first, wbuf[0, j], preferred_element_type=jnp.float32) + jnp.dot(second, wbuf[1, j], preferred_element_type=jnp.float32)

        for j in range(tiles):
            part[:at.size, j * nc:(j + 1) * nc] = product(j)
        for t, side, start in sends:
            encode(ysend, rows_at(t, side), part[start:start + tt, :])
        for t, side, start in sends:
            y_copy(t, side).start()
        if between:
            between()
        for j in range(tiles):
            acc[at, j * nc:(j + 1) * nc] = product(tiles + j)

    def reduce_other(t):
        y_copy(t, 1).wait_recv()
        at = rows_at(t, 1)
        encode(xsend, rows_of(t), acc[at, :] + decode(yrecv, at))
        x_copy(t).start()

    def reduce_own(t):
        y_copy(t, 0).wait_recv()
        at = rows_at(t, 0)
        acc[at, :] += decode(yrecv, at)

    def finish(t):
        x_copy(t).wait_recv()
        o_ref[rows_of(t), :] = (acc[rows_at(t, 0), :] + decode(xrecv, rows_of(t))).astype(o_ref.dtype)

    def finish_own(t):
        within(0, t - LAG_Y, reduce_own)
        within(0, t - LAG_X, finish)

    def reduce(t):
        within(0, t + LEAD - 1 - LAG_O, reduce_other)
        finish_own(t)

    def early(t):
        gather(t)
        multiply(rows_at(t + LEAD, 1), [(t + LEAD, 1, 0)], lambda: halfway(t))
        reduce(t)

    def steady(t):
        gather(t)
        multiply(pl.ds(pl.multiple_of(2 * t * tt, 2 * tt), 2 * tt), [(t + LEAD, 1, tt), (t, 0, 0)], lambda: halfway(t))
        reduce(t)

    def late(t):
        gather(t)
        multiply(rows_at(t, 0), [(t, 0, 0)], lambda: within(0, t + LEAD - 1 - LAG_O, reduce_other))
        finish_own(t)

    w_all(1 - own).wait_recv()
    each(-LEAD, 0, early)
    each(0, PIECES - LEAD, steady)
    each(PIECES - LEAD, PIECES - 2, late)
    gather(PIECES - 2)
    gather(PIECES - 1)
    multiply(pl.ds(2 * (PIECES - 2) * tt, 4 * tt), [(PIECES - 2, 0, 0), (PIECES - 1, 0, 2 * tt)], lambda: reduce_other(PIECES - 1))
    finish_own(PIECES - 2)
    finish_own(PIECES - 1)
    each(PIECES, PIECES + LAG_X, finish_own)

    def sent(sem):
        remote(a_all(0), a_all(0), sem, a_recv.at[0, 0], row=peer).wait_send()

    def sent_few(sem, count):
        if count:
            some = abuf.at[0, pl.ds(0, count * tt), :]
            remote(some, some, sem, a_recv.at[0, 0], row=peer).wait_send()

    few = len(DETOURS)

    @pl.when(u == 0)
    def _():
        sent(f_send.at[0])
        sent(f_send.at[2])
        sent_few(c_send, few)

    @pl.when(u == 1)
    def _():
        for n in range(2):
            sent(f_send.at[n])
            sent(b_send.at[n])
        sent_few(f_send.at[2], PIECES - few)
        sent_few(b_send.at[2], PIECES - SHORT)
        sent_few(b_send.at[3], few)
        sent_few(c_send, few)

    @pl.when(u == 2)
    def _():
        for n in range(2):
            sent(f_send.at[n])
        sent(b_send.at[1])
        sent_few(f_send.at[2], PIECES - few)
        sent_few(f_send.at[3], SHORT)
        sent_few(b_send.at[3], few)

    @pl.when(u == far)
    def _():
        sent_few(b_send.at[3], few)
        sent_few(c_send, SHORT)

    sent(c_send)
    remote(ysend, yrecv, y_send, y_recv.at[0, 0], layer=1 - l).wait_send()
    remote(xsend, xrecv, x_send, x_recv.at[0], row=peer).wait_send()
    w_all(own).wait_send()


def pair_call(rows, cols, attn_values, out_weight):
    tokens, depth = attn_values.shape
    width = out_weight.shape[1]
    half = width // 2
    nc = half // 4
    dma = pltpu.SemaphoreType.DMA
    return pl.pallas_call(
        functools.partial(pair_kernel, rows, cols),
        out_shape=jax.ShapeDtypeStruct((tokens, half), jnp.bfloat16),
        in_specs=[pl.BlockSpec(memory_space=pltpu.HBM)] * 2,
        out_specs=pl.BlockSpec(memory_space=pltpu.VMEM),
        scratch_shapes=[
            pltpu.VMEM((3, 2 * tokens, depth), jnp.bfloat16),
            pltpu.VMEM((2, width // nc, depth, nc), jnp.bfloat16),
            pltpu.VMEM((2 * tokens, half), jnp.float32),
            pltpu.VMEM((4 * tokens // PIECES, half), jnp.float32),
            pltpu.VMEM((2 * tokens, half + 128), jnp.bfloat16),
            pltpu.VMEM((2 * tokens, half + 128), jnp.bfloat16),
            pltpu.VMEM((tokens, half + 128), jnp.bfloat16),
            pltpu.VMEM((tokens, half + 128), jnp.bfloat16),
            dma,
            dma,
            dma((4, PIECES)),
            dma((SHORT + len(DETOURS),)),
            dma((4,)),
            dma((4,)),
            dma,
            dma,
            dma,
            dma,
            dma((PIECES, 2)),
            dma,
            dma((PIECES,)),
        ],
        compiler_params=pltpu.CompilerParams(collective_id=1, has_side_effects=True, vmem_limit_bytes=48 * 2**20),
    )(*(pltpu.with_memory_space_constraint(v, pltpu.HBM) for v in (attn_values, out_weight)))


def pairs_up(rows, cols, attn_values, out_weight):
    groups, depth = rows // 2, attn_values.shape[1]
    same = cols == 2 * groups and depth == out_weight.shape[0]
    whole = attn_values.shape[0] % (16 * PIECES) == 0 and out_weight.shape[1] % 1024 == 0
    return groups == 2 and same and whole


def solution(mesh):
    rows, cols = mesh.shape["row"], mesh.shape["col"]

    def shards(attn_values, out_weight):
        if pairs_up(rows, cols, attn_values, out_weight):
            return pair_call(rows, cols, attn_values, out_weight)
        tokens, depth_a = attn_values.shape
        depth_w, width = out_weight.shape
        nc, jh = width // COLUMN_CHUNKS, COLUMN_CHUNKS // 2
        pieces = COLUMN_CHUNKS - 1 + last_pieces(depth_w)
        dma = pltpu.SemaphoreType.DMA
        return pl.pallas_call(
            functools.partial(kernel, rows, cols),
            out_shape=jax.ShapeDtypeStruct((tokens, width // 2), jnp.bfloat16),
            in_specs=[pl.BlockSpec(memory_space=pltpu.HBM)] * 2,
            out_specs=pl.BlockSpec(memory_space=pltpu.VMEM),
            scratch_shapes=[
                pltpu.VMEM((cols, tokens, depth_a), jnp.bfloat16),
                pltpu.VMEM((COLUMN_CHUNKS, rows * depth_w, nc), jnp.bfloat16),
                pltpu.VMEM((jh, tokens, nc), jnp.float32),
                pltpu.VMEM((jh, tokens, nc), jnp.float32),
                pltpu.VMEM((tokens, nc), jnp.float32),
                dma((TOKEN_CHUNKS,)),
                dma((pieces,)),
                dma((TOKEN_CHUNKS, cols)),
                dma((TOKEN_CHUNKS, cols)),
                dma((TOKEN_CHUNKS, cols)),
                dma((pieces, rows)),
                dma((pieces, rows // 2)),
                dma((pieces, rows // 2)),
                dma((TOKEN_CHUNKS, jh)),
                dma((TOKEN_CHUNKS, jh)),
            ],
            compiler_params=pltpu.CompilerParams(collective_id=0, has_side_effects=True, vmem_limit_bytes=48 * 2**20),
        )(*(pltpu.with_memory_space_constraint(x, pltpu.HBM) for x in (attn_values, out_weight)))

    in_specs = (P("row", ("layer", "col")), P(("layer", "row"), "col"))
    out_specs = P("row", ("col", "layer"))
    return jax.shard_map(shards, mesh=mesh, in_specs=in_specs, out_specs=out_specs, check_vma=False)
```

```python
import functools

import jax
import jax.numpy as jnp
from jax import lax
from jax.experimental import pallas as pl
from jax.experimental.pallas import tpu as pltpu
from jax.sharding import PartitionSpec as P

TOKEN_CHUNKS = 4
COLUMN_CHUNKS = 8


def last_pieces(depth_w):
    return max(1, min(4, depth_w // 256))


def schedule(token_chunks, column_chunks, col_count):
    events = []
    for t in range(token_chunks):
        for d in range(1, col_count):
            at = (col_count - 1) * t + (1 if d == 1 else d + 1)
            events.append((at, 0, t, d))
    span = (col_count - 1) * token_chunks * 4 / 3
    for j in range(column_chunks - 1):
        events.append((span * (j + 1) / column_chunks, 1, j, 0))
    ordered, clock = [], 0
    for at, kind, first, second in sorted(events, key=lambda e: (e[1], e[2], e[3])):
        if kind == 0:
            clock = max(clock, at)
            at = clock
        ordered.append((at, kind, first, second))
    return sorted(ordered)


def kernel(rows, cols, a_ref, w_ref, o_ref, abuf, wbuf, ysend, yrecv, early, loc_a, loc_w, a_recv, a_right, a_left, w_recv, w_send, p_send, y_recv, y_send):
    r, c, l = lax.axis_index("row"), lax.axis_index("col"), lax.axis_index("layer")
    groups = rows // 2
    core, group = lax.rem(r, 2), r // 2
    partner = 2 * group + 1 - core
    tokens, depth_a = a_ref.shape
    depth_w, width = w_ref.shape
    tt, half = tokens // TOKEN_CHUNKS, width // 2
    nc, jh = width // COLUMN_CHUNKS, COLUMN_CHUNKS // 2
    last, cuts = COLUMN_CHUNKS - 1, last_pieces(depth_w)
    pieces = last + cuts

    def piece(p):
        return (p, 0, depth_w) if p < last else (last, (p - last) * depth_w // cuts, depth_w // cuts)

    def peer(g):
        return 2 * lax.rem(group + g + groups, groups) + core

    def a_at(block, t):
        return abuf.at[block, pl.ds(t * tt, tt), :]

    def w_at(row, p):
        j, start, count = piece(p)
        return wbuf.at[j, pl.ds(pl.multiple_of(row * depth_w + start, count), count), :]

    def own_a(t):
        return pltpu.make_async_copy(a_ref.at[pl.ds(t * tt, tt), :], a_at(c, t), loc_a.at[t])

    def own_w(p):
        j, start, count = piece(p)
        side = 1 - l if j < jh else l
        at = pl.multiple_of(side * half + (j % jh) * nc, nc)
        return pltpu.make_async_copy(w_ref.at[pl.ds(start, count), pl.ds(at, nc)], w_at(r, p), loc_w.at[p])

    def a_copy(block, t, to, sems):
        return pltpu.make_async_remote_copy(a_at(block, t), a_at(block, t), sems.at[t, block], a_recv.at[t, block], device_id={"col": to})

    def w_copy(row, j, to, sem):
        return pltpu.make_async_remote_copy(w_at(row, j), w_at(row, j), sem, w_recv.at[j, row], device_id={"row": to})

    def y_copy(t, j):
        rows_t = pl.ds(t * tt, tt)
        return pltpu.make_async_remote_copy(ysend.at[j, rows_t, :], yrecv.at[j, rows_t, :], y_send.at[t, j], y_recv.at[t, j], device_id={"layer": 1 - l})

    def right(block, t):
        return a_copy(block, t, c + 1, a_right)

    def left(block, t):
        return a_copy(block, t, c - 1, a_left)

    for n in range(max(TOKEN_CHUNKS, pieces)):
        if n < pieces:
            own_w(n).start()
        if n < TOKEN_CHUNKS:
            own_a(n).start()

    has_right, has_left = c < cols - 1, c > 0
    barrier = pltpu.get_barrier_semaphore()

    def greet(device_id):
        pl.semaphore_signal(barrier, inc=1, device_id=device_id)

    greet({"row": partner})
    greet({"layer": 1 - l})
    for g in range(1, groups):
        greet({"row": peer(g)})
    pl.when(has_right)(lambda: greet({"col": c + 1}))
    pl.when(has_left)(lambda: greet({"col": c - 1}))
    pl.semaphore_wait(barrier, 1 + groups + has_right.astype(jnp.int32) + has_left.astype(jnp.int32))

    def send_a(t):
        own_a(t).wait()
        pl.when(has_right)(lambda: right(c, t).start())
        pl.when(has_left)(lambda: left(c, t).start())

    def send_w(j):
        own_w(j).wait()
        for g in range(1, groups):
            w_copy(r, j, peer(g), w_send.at[j, g]).start()
        w_copy(r, j, partner, p_send.at[j, 0]).start()

    send_w(0)
    send_a(0)
    send_a(1)
    for p in range(1, pieces):
        send_w(p)

    def take_a(t, d):
        @pl.when(c >= d)
        def _():
            right(c - d, t).wait_recv()
            pl.when(has_right)(lambda: right(c - d, t).start())

        @pl.when(c + d < cols)
        def _():
            left(c + d, t).wait_recv()
            pl.when(has_left)(lambda: left(c + d, t).start())

        if d == cols - 1 and t + 2 < TOKEN_CHUNKS:
            send_a(t + 2)

    def take_w(j):
        for g in range(1, groups):
            source = peer(-g)
            w_copy(source, j, partner, p_send.at[j, g]).wait_recv()
            w_copy(source, j, partner, p_send.at[j, g]).start()

    def take_partner(j):
        for g in range(groups):
            source = 2 * g + 1 - core
            w_copy(source, j, partner, p_send.at[j, 0]).wait_recv()

    def product(rows_t, j):
        total = jnp.dot(abuf[0, rows_t, :], wbuf[j, pl.ds(0, depth_a), :], preferred_element_type=jnp.float32)
        for block in range(1, cols):
            total += jnp.dot(abuf[block, rows_t, :], wbuf[j, pl.ds(block * depth_a, depth_a), :], preferred_element_type=jnp.float32)
        return total

    def partials(tiles):
        t0, j0 = tiles[0]
        wide = 1 + tiles[-1][1] - j0

        def one(n, carry):
            t, j = t0 + n // wide, j0 + lax.rem(n, wide)
            rows_t = pl.ds(pl.multiple_of(t * tt, tt), tt)
            ysend[j, rows_t, :] = product(rows_t, j)
            return carry

        def send(n, carry):
            y_copy(t0 + n // wide, j0 + lax.rem(n, wide)).start()
            return carry

        lax.fori_loop(0, len(tiles), one, 0)
        lax.fori_loop(0, len(tiles), send, 0)

    def finish(j):
        def one(t, carry):
            rows_t = pl.ds(pl.multiple_of(t * tt * 2, tt * 2), tt * 2)
            y_copy(2 * t, j - jh).wait_recv()
            y_copy(2 * t + 1, j - jh).wait_recv()
            o_ref[rows_t, (j - jh) * nc:(j - jh + 1) * nc] = (product(rows_t, j) + yrecv[j - jh, rows_t, :]).astype(o_ref.dtype)
            return carry

        lax.fori_loop(0, TOKEN_CHUNKS // 2, one, 0)

    def part(j, rows_t, start, count):
        columns = pl.ds(pl.multiple_of(lax.rem(start, depth_a), min(count, depth_a)), count)
        weights = wbuf[j, pl.ds(pl.multiple_of(start, count), count), :]
        return jnp.dot(abuf[start // depth_a, rows_t, columns], weights, preferred_element_type=jnp.float32)

    def each_rows(body):
        def one(t, carry):
            body(pl.ds(pl.multiple_of(t * tt * 2, tt * 2), tt * 2))
            return carry

        lax.fori_loop(0, TOKEN_CHUNKS // 2, one, 0)

    def take_own_rows():
        for h in range(cuts):
            w_copy(partner, last + h, partner, p_send.at[last + h, 0]).wait_recv()
        count = min(depth_w, depth_a)
        for n in range(depth_w // count):
            @each_rows
            def _(rows_t):
                total = part(last, rows_t, r * depth_w + n * count, count) + part(last, rows_t, partner * depth_w + n * count, count)
                early[rows_t, :] = total if n == 0 else early[rows_t, :] + total

    def finish_last():
        count = depth_w // cuts
        for t in range(TOKEN_CHUNKS):
            y_copy(t, jh - 1).wait_recv()
        for h in range(cuts):
            take_w(last + h)
            for g in range(1, groups):
                own, other = peer(-g), peer(-g) + 1 - 2 * core

                @each_rows
                def _(rows_t):
                    early[rows_t, :] += part(last, rows_t, own * depth_w + h * count, count)

                w_copy(other, last + h, partner, p_send.at[last + h, 0]).wait_recv()

                @each_rows
                def _(rows_t):
                    total = early[rows_t, :] + part(last, rows_t, other * depth_w + h * count, count)
                    if h < cuts - 1 or g < groups - 1:
                        early[rows_t, :] = total
                    else:
                        o_ref[rows_t, (jh - 1) * nc:jh * nc] = (total + yrecv[jh - 1, rows_t, :]).astype(o_ref.dtype)

    got_t, got_j, done_own, own_rows = 0, 0, jh, False
    for _, kind, first, second in schedule(TOKEN_CHUNKS, COLUMN_CHUNKS, cols):
        if kind == 0:
            take_a(first, second)
            if second == cols - 1:
                got_t = first + 1
                if got_j:
                    partials([(first, j) for j in range(min(got_j, jh))])
        else:
            if first == last - 1 and got_t == TOKEN_CHUNKS:
                take_own_rows()
                own_rows = True
            take_w(first)
            take_partner(first)
            got_j = first + 1
            if first < jh and got_t:
                partials([(t, first) for t in range(got_t)])
        while got_t == TOKEN_CHUNKS and done_own < got_j:
            finish(done_own)
            done_own += 1
    if not own_rows:
        take_own_rows()
    finish_last()

    for t in range(TOKEN_CHUNKS):
        for block in range(cols):
            @pl.when(has_right & (block <= c))
            def _():
                right(block, t).wait_send()

            @pl.when(has_left & (block >= c))
            def _():
                left(block, t).wait_send()

        for j in range(jh):
            y_copy(t, j).wait_send()
    for p in range(pieces):
        for g in range(groups):
            w_copy(r, p, partner, p_send.at[p, g]).wait_send()
            if g:
                w_copy(r, p, partner, w_send.at[p, g]).wait_send()


PIECES = 16
DETOURS = ((12, 0, 6), (14, 1, 8))
SHORT = 3
FILL = 6
FILL_BACK = 3
LEAD = 3
LAG_O = 1
LAG_Y = 2
LAG_X = 5
SPAN = 250.0


def pair_kernel(rows, cols, a_ref, w_ref, o_ref, abuf, wbuf, acc, part, ysend, yrecv, xsend, xrecv, loc_a, loc_w, a_recv, o_recv, f_send, b_send, c_send, w_send, w_recv, y_send, y_recv, x_send, x_recv):
    r, c, l = lax.axis_index("row"), lax.axis_index("col"), lax.axis_index("layer")
    x, core = r // 2, lax.rem(r, 2)
    partner, peer = 2 * x + 1 - core, 2 * (1 - x) + core
    step, u, far = 1 - 2 * x, c + x * (cols - 1 - 2 * c), cols - 1
    own = core + x * (1 - 2 * core)
    tokens, depth = a_ref.shape
    half = w_ref.shape[1] // 2
    tt, nc = tokens // PIECES, wbuf.shape[3]
    tiles = half // nc

    def rows_at(t, side):
        at = 2 * t if side == 0 else 2 * lax.rem(t + PIECES - LEAD, PIECES) + 1
        return pl.ds(pl.multiple_of(at * tt, tt), tt)

    def rows_of(t):
        return pl.ds(pl.multiple_of(t * tt, tt), tt)

    def a_at(v, side, t):
        return abuf.at[v, rows_at(t, side), :]

    def a_all(v):
        return abuf.at[v, pl.ds(0, tokens), :]

    def own_a(t):
        return pltpu.make_async_copy(a_ref.at[rows_of(t), :], a_at(u - u // far, 0, t), loc_a)

    def own_w(j):
        side = 1 - l if j < tiles else l
        at = pl.multiple_of(side * half + (j % tiles) * nc, nc)
        return pltpu.make_async_copy(w_ref.at[:, pl.ds(at, nc)], wbuf.at[own, j], loc_w)

    def remote(source, target, sent, got, **device):
        return pltpu.make_async_remote_copy(source, target, sent, got, device_id=device)

    def w_all(slot):
        return remote(wbuf.at[slot], wbuf.at[slot], w_send, w_recv, row=partner)

    def ahead(v, side, t):
        return remote(a_at(v, side, t), a_at(v, side, t), f_send.at[v + 2 * side], a_recv.at[v + 2 * side, t], col=c + step)

    def back(v, side, t):
        return remote(a_at(v, side, t), a_at(v, side, t), b_send.at[v - 1 + 2 * side], a_recv.at[u - 1 if v == 2 else v + 2 * side, t], col=c - step)

    def across(t):
        to = 1 - u // far
        return remote(a_at(2, 0, t), a_at(to, 1, t), c_send, a_recv.at[to + 2, t], row=peer)

    def slot(t):
        return t if t < SHORT else SHORT + [n for n, _, _ in DETOURS].index(t)

    def leave(t):
        return remote(a_at(2, 0, t), a_at(2, 1, t), b_send.at[3], o_recv.at[slot(t)], col=c - step)

    def enter(t):
        return remote(a_at(2, 0, t), a_at(2, 1, t), f_send.at[3], o_recv.at[slot(t)], col=c + step)

    def back_other(t):
        return remote(a_at(2, 1, t), a_at(2, 1, t), b_send.at[3], o_recv.at[slot(t)], col=c - step)

    def over(t):
        to = u // far
        return remote(a_at(2, 1, t), a_at(to, 1, t), c_send, a_recv.at[to + 2, t], row=peer)

    def y_copy(t, side):
        at = rows_at(t, side)
        return remote(ysend.at[at, :], yrecv.at[at, :], y_send, y_recv.at[t, side], layer=1 - l)

    def x_copy(t):
        at = rows_of(t)
        return remote(xsend.at[at, :], xrecv.at[at, :], x_send, x_recv.at[t], row=peer)

    def take(v, side, t):
        ahead(v, side, t).wait_recv()

    def take_away(t):
        remote(a_at(2, 0, t), a_at(2, 0, t), b_send.at[1], a_recv.at[u, t], col=c - step).wait_recv()

    def take_other(t):
        enter(t).wait_recv()

    def within(first, t, body):
        if isinstance(t, int):
            if first <= t < PIECES:
                body(t)
        else:
            pl.when((t >= first) & (t < PIECES))(lambda: body(t))

    for t in range(PIECES):
        own_a(t).start()

    has_next, has_last = u < far, u > 0
    barrier = pltpu.get_barrier_semaphore()

    def greet(device_id):
        pl.semaphore_signal(barrier, inc=1, device_id=device_id)

    greet({"row": partner})
    greet({"row": peer})
    greet({"layer": 1 - l})
    pl.when(has_next)(lambda: greet({"col": c + step}))
    pl.when(has_last)(lambda: greet({"col": c - step}))
    pl.semaphore_wait(barrier, 3 + has_next.astype(jnp.int32) + has_last.astype(jnp.int32))

    pltpu.make_async_copy(a_ref, a_all(u - u // far), loc_a).wait()

    def send_first(t):
        ahead(0, 0, t).start()

    def send_ahead(t):
        ahead(1, 0, t).start()

    def send_back(t):
        back(1, 0, t).start()

    def each(start, stop, body):
        def one(t, carry):
            body(t)
            return carry

        lax.fori_loop(start, stop, one, 0)

    def both(t):
        across(t).start()
        back(2, 0, t).start()

    @pl.when(u == 0)
    def _():
        each(0, 2, send_first)

    @pl.when(u == 1)
    def _():
        for t in range(FILL):
            send_ahead(t)
            if t < FILL_BACK:
                send_back(t)

    @pl.when(u == 2)
    def _():
        for t in range(SHORT):
            enter(t).start()

        each(0, FILL, both)

    @pl.when(u == far)
    def _():
        for t, _, _ in DETOURS:
            leave(t).start()
        each(0, 4, lambda t: across(t).start())

    for j in range(2 * tiles):
        own_w(j).start()
    pltpu.make_async_copy(wbuf.at[1 - own], wbuf.at[own], loc_w).wait()
    w_all(own).start()

    def on(v, side):
        def body(t):
            take(v, side, t)
            ahead(v, side, t).start()

        return body

    def unless(t, skipped, body):
        if isinstance(t, int):
            if t not in skipped:
                body()
        elif skipped:
            pl.when(functools.reduce(jnp.logical_and, [t != n for n in skipped]))(body)
        else:
            body()

    def on_most(t):
        take(0, 1, t)
        unless(t, [n for n, _, _ in DETOURS], lambda: ahead(0, 1, t).start())

    def on_back(t):
        take_other(t)
        back_other(t).start()

    def cross(t):
        take_away(t)
        across(t).start()

    def away(t):
        take_away(t)
        back(2, 0, t).start()
        across(t).start()

    def pass_back(t):
        within(1, t + 1, away)
        take(1, 1, t)
        unless(t, list(range(SHORT)), lambda: back(1, 1, t).start())

    @pl.when(u == 0)
    def _():
        for t in range(4):
            on(0, 1)(t)
            if t >= 2:
                send_first(t)
        cross(0)

    @pl.when(u == 1)
    def _():
        away(0)
        for t in range(3):
            pass_back(t)
        for t in range(2):
            on_most(t)

    @pl.when(u == 2)
    def _():
        for t in range(FILL):
            on(1, 0)(t)
            if t == 1:
                for n, _, _ in DETOURS:
                    on_back(n)
                each(FILL, PIECES, both)
        on_most(0)

    @pl.when(u == far)
    def _():
        for t in range(SHORT):
            take_other(t)
            over(t).start()
        each(4, PIECES, lambda t: across(t).start())

    def gather(t):
        @pl.when(u == 0)
        def _():
            for n, _, at in DETOURS:
                @pl.when(t == at)
                def _():
                    take_other(n)
                    over(n).start()

            within(1, t + LEAD + 1, cross)
            within(4, t + LEAD + 4, on(0, 1))
            within(4, t + 4, send_first)
            within(0, t + LEAD, lambda t: take(1, 1, t))
            within(0, t, lambda t: take(1, 0, t))

        @pl.when(u == 1)
        def _():
            for n, at, _ in DETOURS:
                @pl.when(t == at)
                def _():
                    on_back(n)
                    over(n).start()

            within(3, t + LEAD + 3, pass_back)
            within(FILL_BACK, t + 3, send_back)
            within(2, t + LEAD + 2, on_most)
            within(0, t + 2, on(0, 0))
            within(FILL, t + 2, send_ahead)

        @pl.when(u == 2)
        def _():
            within(0, t, on(0, 0))
            within(FILL, t, on(1, 0))
            within(0, t + LEAD, lambda t: take(1, 1, t))

        @pl.when(u == far)
        def _():
            within(0, t + LEAD, lambda t: take(0, 1, t))
            within(0, t + LEAD, lambda t: take(1, 1, t))
            within(0, t, lambda t: take(0, 0, t))
            within(0, t, lambda t: take(1, 0, t))

    def halfway(t):
        pl.when(u == 2)(lambda: within(0, t + LEAD + 1, on_most))

    def encode(ref, at, value):
        scale = jnp.maximum(1.01 * jnp.max(jnp.abs(value), axis=1, keepdims=True), 1e-30).astype(jnp.bfloat16)
        level = jnp.exp2(jnp.abs(value) * (SPAN / scale.astype(jnp.float32)) - SPAN / 2)
        ref[at, :half] = jnp.where(value < 0, -level, level).astype(jnp.bfloat16)
        ref[at, half:] = jnp.broadcast_to(scale, (value.shape[0], ref.shape[1] - half))

    def decode(ref, at):
        level = ref[at, :half].astype(jnp.float32)
        scale = ref[at, half:half + 1].astype(jnp.float32)
        share = jnp.log2(jnp.abs(level)) * (1 / SPAN) + 0.5
        return jnp.where(level < 0, -share, share) * scale

    def multiply(at, sends, between=None):
        first, second = abuf[0, at, :], abuf[1, at, :]

        def product(j):
            return jnp.dot(first, wbuf[0, j], preferred_element_type=jnp.float32) + jnp.dot(second, wbuf[1, j], preferred_element_type=jnp.float32)

        for j in range(tiles):
            part[:at.size, j * nc:(j + 1) * nc] = product(j)
        for t, side, start in sends:
            encode(ysend, rows_at(t, side), part[start:start + tt, :])
        for t, side, start in sends:
            y_copy(t, side).start()
        if between:
            between()
        for j in range(tiles):
            acc[at, j * nc:(j + 1) * nc] = product(tiles + j)

    def reduce_other(t):
        y_copy(t, 1).wait_recv()
        at = rows_at(t, 1)
        encode(xsend, rows_of(t), acc[at, :] + decode(yrecv, at))
        x_copy(t).start()

    def reduce_own(t):
        y_copy(t, 0).wait_recv()
        at = rows_at(t, 0)
        acc[at, :] += decode(yrecv, at)

    def finish(t):
        x_copy(t).wait_recv()
        o_ref[rows_of(t), :] = (acc[rows_at(t, 0), :] + decode(xrecv, rows_of(t))).astype(o_ref.dtype)

    def finish_own(t):
        within(0, t - LAG_Y, reduce_own)
        within(0, t - LAG_X, finish)

    def reduce(t):
        within(0, t + LEAD - 1 - LAG_O, reduce_other)
        finish_own(t)

    def early(t):
        gather(t)
        multiply(rows_at(t + LEAD, 1), [(t + LEAD, 1, 0)], lambda: halfway(t))
        reduce(t)

    def steady(t):
        gather(t)
        multiply(pl.ds(pl.multiple_of(2 * t * tt, 2 * tt), 2 * tt), [(t + LEAD, 1, tt), (t, 0, 0)], lambda: halfway(t))
        reduce(t)

    def late(t):
        gather(t)
        multiply(rows_at(t, 0), [(t, 0, 0)], lambda: within(0, t + LEAD - 1 - LAG_O, reduce_other))
        finish_own(t)

    w_all(1 - own).wait_recv()
    each(-LEAD, 0, early)
    each(0, PIECES - LEAD, steady)
    each(PIECES - LEAD, PIECES - 2, late)
    gather(PIECES - 2)
    gather(PIECES - 1)
    multiply(pl.ds(2 * (PIECES - 2) * tt, 4 * tt), [(PIECES - 2, 0, 0), (PIECES - 1, 0, 2 * tt)], lambda: reduce_other(PIECES - 1))
    finish_own(PIECES - 2)
    finish_own(PIECES - 1)
    each(PIECES, PIECES + LAG_X, finish_own)

    def sent(sem):
        remote(a_all(0), a_all(0), sem, a_recv.at[0, 0], row=peer).wait_send()

    def sent_few(sem, count):
        if count:
            some = abuf.at[0, pl.ds(0, count * tt), :]
            remote(some, some, sem, a_recv.at[0, 0], row=peer).wait_send()

    few = len(DETOURS)

    @pl.when(u == 0)
    def _():
        sent(f_send.at[0])
        sent(f_send.at[2])
        sent_few(c_send, few)

    @pl.when(u == 1)
    def _():
        for n in range(2):
            sent(f_send.at[n])
            sent(b_send.at[n])
        sent_few(f_send.at[2], PIECES - few)
        sent_few(b_send.at[2], PIECES - SHORT)
        sent_few(b_send.at[3], few)
        sent_few(c_send, few)

    @pl.when(u == 2)
    def _():
        for n in range(2):
            sent(f_send.at[n])
        sent(b_send.at[1])
        sent_few(f_send.at[2], PIECES - few)
        sent_few(f_send.at[3], SHORT)
        sent_few(b_send.at[3], few)

    @pl.when(u == far)
    def _():
        sent_few(b_send.at[3], few)
        sent_few(c_send, SHORT)

    sent(c_send)
    remote(ysend, yrecv, y_send, y_recv.at[0, 0], layer=1 - l).wait_send()
    remote(xsend, xrecv, x_send, x_recv.at[0], row=peer).wait_send()
    w_all(own).wait_send()


def pair_call(rows, cols, attn_values, out_weight):
    tokens, depth = attn_values.shape
    width = out_weight.shape[1]
    half = width // 2
    nc = half // 4
    dma = pltpu.SemaphoreType.DMA
    return pl.pallas_call(
        functools.partial(pair_kernel, rows, cols),
        out_shape=jax.ShapeDtypeStruct((tokens, half), jnp.bfloat16),
        in_specs=[pl.BlockSpec(memory_space=pltpu.HBM)] * 2,
        out_specs=pl.BlockSpec(memory_space=pltpu.VMEM),
        scratch_shapes=[
            pltpu.VMEM((3, 2 * tokens, depth), jnp.bfloat16),
            pltpu.VMEM((2, width // nc, depth, nc), jnp.bfloat16),
            pltpu.VMEM((2 * tokens, half), jnp.float32),
            pltpu.VMEM((4 * tokens // PIECES, half), jnp.float32),
            pltpu.VMEM((2 * tokens, half + 128), jnp.bfloat16),
            pltpu.VMEM((2 * tokens, half + 128), jnp.bfloat16),
            pltpu.VMEM((tokens, half + 128), jnp.bfloat16),
            pltpu.VMEM((tokens, half + 128), jnp.bfloat16),
            dma,
            dma,
            dma((4, PIECES)),
            dma((SHORT + len(DETOURS),)),
            dma((4,)),
            dma((4,)),
            dma,
            dma,
            dma,
            dma,
            dma((PIECES, 2)),
            dma,
            dma((PIECES,)),
        ],
        compiler_params=pltpu.CompilerParams(collective_id=1, has_side_effects=True, vmem_limit_bytes=48 * 2**20),
    )(*(pltpu.with_memory_space_constraint(v, pltpu.HBM) for v in (attn_values, out_weight)))


def pairs_up(rows, cols, attn_values, out_weight):
    groups, depth = rows // 2, attn_values.shape[1]
    same = cols == 2 * groups and depth == out_weight.shape[0]
    whole = attn_values.shape[0] % (16 * PIECES) == 0 and out_weight.shape[1] % 1024 == 0
    return groups == 2 and same and whole


def solution(mesh):
    rows, cols = mesh.shape["row"], mesh.shape["col"]

    def shards(attn_values, out_weight):
        if pairs_up(rows, cols, attn_values, out_weight):
            return pair_call(rows, cols, attn_values, out_weight)
        tokens, depth_a = attn_values.shape
        depth_w, width = out_weight.shape
        nc, jh = width // COLUMN_CHUNKS, COLUMN_CHUNKS // 2
        pieces = COLUMN_CHUNKS - 1 + last_pieces(depth_w)
        dma = pltpu.SemaphoreType.DMA
        return pl.pallas_call(
            functools.partial(kernel, rows, cols),
            out_shape=jax.ShapeDtypeStruct((tokens, width // 2), jnp.bfloat16),
            in_specs=[pl.BlockSpec(memory_space=pltpu.HBM)] * 2,
            out_specs=pl.BlockSpec(memory_space=pltpu.VMEM),
            scratch_shapes=[
                pltpu.VMEM((cols, tokens, depth_a), jnp.bfloat16),
                pltpu.VMEM((COLUMN_CHUNKS, rows * depth_w, nc), jnp.bfloat16),
                pltpu.VMEM((jh, tokens, nc), jnp.float32),
                pltpu.VMEM((jh, tokens, nc), jnp.float32),
                pltpu.VMEM((tokens, nc), jnp.float32),
                dma((TOKEN_CHUNKS,)),
                dma((pieces,)),
                dma((TOKEN_CHUNKS, cols)),
                dma((TOKEN_CHUNKS, cols)),
                dma((TOKEN_CHUNKS, cols)),
                dma((pieces, rows)),
                dma((pieces, rows // 2)),
                dma((pieces, rows // 2)),
                dma((TOKEN_CHUNKS, jh)),
                dma((TOKEN_CHUNKS, jh)),
            ],
            compiler_params=pltpu.CompilerParams(collective_id=0, has_side_effects=True, vmem_limit_bytes=48 * 2**20),
        )(*(pltpu.with_memory_space_constraint(x, pltpu.HBM) for x in (attn_values, out_weight)))

    in_specs = (P("row", ("layer", "col")), P(("layer", "row"), "col"))
    out_specs = P("row", ("col", "layer"))
    return jax.shard_map(shards, mesh=mesh, in_specs=in_specs, out_specs=out_specs, check_vma=False)
```
